32 devices in a mesh: dp: 2 (over y), tm: 16 (over z, x, core).
Axes of the slice: x: 2, y: 2, z: 4, core: 2. Of those that a mesh axis runs over, the one named last changes fastest.
Arguments:
- inputs: bfloat16 [2, 128, 14, 14, 512], P('dp', 'tm'), may hold values from -6 to 6
- clip_ids: int32 [2, 128], P('dp'), may hold values from 0 to 15, as said below
- norm1_gain: bfloat16 [2, 512], replicated, may hold values from 0.5 to 1.5
- norm1_bias: bfloat16 [2, 512], replicated, may hold values from -1.75 to 1.75
- qkv_weight: bfloat16 [2, 512, 1536], replicated, may hold values from -0.25 to 0.25
- q_bias: bfloat16 [2, 512], replicated, may hold values from -3 to 3
- v_bias: bfloat16 [2, 512], replicated, may hold values from -3 to 3
- bias_table: bfloat16 [2, 2535, 16], replicated, may hold values from -6 to 6
- proj_weight: bfloat16 [2, 512, 512], replicated, may hold values from -2 to 2
- proj_bias: bfloat16 [2, 512], replicated, may hold values from -1.75 to 1.75
- norm2_gain: bfloat16 [2, 512], replicated, may hold values from 0.5 to 1.5
- norm2_bias: bfloat16 [2, 512], replicated, may hold values from -1.75 to 1.75
- fc1_weight: bfloat16 [2, 512, 2048], replicated, may hold values from -0.25 to 0.25
- fc1_bias: bfloat16 [2, 2048], replicated, may hold values from -3 to 3
- fc2_weight: bfloat16 [2, 2048, 512], replicated, may hold values from -0.125 to 0.125
- fc2_bias: bfloat16 [2, 512], replicated, may hold values from -1.75 to 1.75
- cotangent: bfloat16 [2, 128, 14, 14, 512], P('dp', 'tm'), may hold values from -6 to 6
Outputs:
- block_output: bfloat16 [2, 128, 14, 14, 512], P('dp', 'tm')
- input_grad: bfloat16 [2, 128, 14, 14, 512], P('dp', 'tm')
- norm1_gain_grad: float32 [2, 512], replicated
- norm1_bias_grad: float32 [2, 512], replicated
- qkv_weight_grad: float32 [2, 512, 1536], P(None, 'tm')
- q_bias_grad: float32 [2, 512], replicated
- v_bias_grad: float32 [2, 512], replicated
- bias_table_grad: float32 [2, 2535, 16], replicated
- proj_weight_grad: float32 [2, 512, 512], P(None, 'tm')
- proj_bias_grad: float32 [2, 512], replicated
- norm2_gain_grad: float32 [2, 512], replicated
- norm2_bias_grad: float32 [2, 512], replicated
- fc1_weight_grad: float32 [2, 512, 2048], P(None, 'tm')
- fc1_bias_grad: float32 [2, 2048], replicated
- fc2_weight_grad: float32 [2, 2048, 512], P(None, 'tm')
- fc2_bias_grad: float32 [2, 512], replicated
The draws below stay inside these ranges and needn't reach their ends.
Inputs may be any that keep to these rules, and one draw needn't show every extreme that they name: `clip_ids`: in each group a clip's number is the index of its first block of 8 token frames; every clip starts at a multiple of 8 token frames and has 8, 16 or 32 of them, except that the group's last 8 token frames always form a clip of their own and the clip before them may be shorter.
All inputs are finite; a program needn't handle non-finite values.
Results may differ from the reference program's by a relative error of at most 0.015.
Values may be sent and summed in bfloat16 or wider, within the bound.
A program may use at most 384 MiB of HBM per device.

```python
import jax
import jax.numpy as jnp
from jax import lax

D = 512
HEADS = 16
HEAD_DIM = 32
FF = 2048
SIDE = 14
WIN_T = 8
WIN_S = 7
SHIFT_T = 4
SHIFT_S = 3
LAYERS = 2
WIN_ROWS = 392
TABLE_ROWS = 2535
GROUPS = 2
FRAMES = 128


def draw_clip_ids(key, part):
    block_count = FRAMES // WIN_T

    def one_group(group_key):
        picked = jax.random.randint(group_key, (block_count,), 0, 3)
        lengths = jnp.array([1, 2, 4], jnp.int32)[picked]
        starts = jnp.cumsum(lengths) - lengths
        positions = jnp.arange(block_count, dtype=jnp.int32)
        reached = starts[None, :] <= positions[:, None]
        block_start = jnp.max(jnp.where(reached, starts[None, :], 0), axis=1)
        block_start = jnp.where(positions == block_count - 1, block_count - 1, block_start)
        return jnp.repeat(block_start, WIN_T)
    return jax.vmap(one_group)(jax.random.split(key, GROUPS)).astype(jnp.int32)


def block_scale(rng, dims, shards, least, high):
    factor_of, own = 1.0, jax.random.fold_in(rng, 6)
    for dim, parts in shards:
        heights = jnp.exp(jax.random.uniform(jax.random.fold_in(own, dim), (parts,), jnp.float32, least / len(shards), high / len(shards)))
        factor_of = factor_of * jnp.repeat(heights, dims[dim] // parts).reshape([-1 if axis == dim else 1 for axis in range(len(dims))])
    return factor_of


def scatter_about(key, extent, deviation, bound, cuts=(), kind=jnp.bfloat16):
    factor_of = block_scale(key, extent, cuts, -0.22, 0.18) if cuts else 1.0
    values = jax.random.normal(key, extent, jnp.float32) * deviation * factor_of
    return jnp.minimum(jnp.maximum(values, -bound), bound).astype(kind)


def setup_inputs(seed: int = 0) -> dict:
    arg_keys = jax.random.split(jax.random.key(seed), 18)
    return {
        "inputs": scatter_about(arg_keys[0], (GROUPS, FRAMES, SIDE, SIDE, D), 1.0, 6.0, ((0, 2), (1, 16))),
        "clip_ids": draw_clip_ids(jax.random.fold_in(arg_keys[17], 71), 0),
        "norm1_gain": jnp.clip(1.0 + 0.1 * jax.random.normal(arg_keys[2], (LAYERS, D), jnp.float32), 0.5, 1.5).astype(jnp.bfloat16),
        "norm1_bias": scatter_about(arg_keys[3], (LAYERS, D), 0.3, 1.75),
        "qkv_weight": scatter_about(arg_keys[4], (LAYERS, D, 3 * D), D ** -0.5, 0.25),
        "q_bias": scatter_about(arg_keys[5], (LAYERS, D), 0.5, 3.0),
        "v_bias": scatter_about(arg_keys[6], (LAYERS, D), 0.5, 3.0),
        "bias_table": scatter_about(arg_keys[7], (LAYERS, TABLE_ROWS, HEADS), 1.0, 6.0),
        "proj_weight": scatter_about(arg_keys[8], (LAYERS, D, D), (max(D // 64, 1)) ** -0.5, 2.0),
        "proj_bias": scatter_about(arg_keys[9], (LAYERS, D), 0.3, 1.75),
        "norm2_gain": jnp.clip(1.0 + 0.1 * jax.random.normal(arg_keys[10], (LAYERS, D), jnp.float32), 0.5, 1.5).astype(jnp.bfloat16),
        "norm2_bias": scatter_about(arg_keys[11], (LAYERS, D), 0.3, 1.75),
        "fc1_weight": scatter_about(arg_keys[12], (LAYERS, D, FF), D ** -0.5, 0.25),
        "fc1_bias": scatter_about(arg_keys[13], (LAYERS, FF), 0.5, 3.0),
        "fc2_weight": scatter_about(arg_keys[14], (LAYERS, FF, D), FF ** -0.5, 0.125),
        "fc2_bias": scatter_about(arg_keys[15], (LAYERS, D), 0.3, 1.75),
        "cotangent": scatter_about(arg_keys[16], (GROUPS, FRAMES, SIDE, SIDE, D), 1.0, 6.0, ((0, 2), (1, 16))),
    }


@jax.custom_vjp
def low(v):
    return lax.optimization_barrier(v.astype(jnp.bfloat16)).astype(jnp.float32)

@jax.custom_vjp
def low_back(v):
    return v

def low_keep(v):
    return (low(v), None)

def low_pass(kept, grad):
    return (grad,)

def back_keep(v):
    return (v, None)

def back_low(kept, grad):
    return (low(grad),)
low.defvjp(low_keep, low_pass)
low_back.defvjp(back_keep, back_low)

def layer_norm(values, gain_row, shift_row):
    center = values - lax.optimization_barrier(jnp.mean(values, axis=-1, keepdims=True))
    spread = lax.optimization_barrier(jnp.mean(center * center, axis=-1, keepdims=True))
    return center * lax.rsqrt(spread + 1e-05) * gain_row + shift_row

def product_high(left_side, right_side):
    return jnp.einsum('...i,ij->...j', left_side, right_side, precision=lax.Precision.HIGHEST)

def relative_index():
    position = jnp.arange(WIN_ROWS, dtype=jnp.int32)
    time_pos = position // (WIN_S * WIN_S)
    high_pos = position // WIN_S % WIN_S
    wide_pos = position % WIN_S
    span_side = 2 * WIN_S - 1
    time_diff = time_pos[:, None] - time_pos[None, :] + (WIN_T - 1)
    high_diff = high_pos[:, None] - high_pos[None, :] + (WIN_S - 1)
    wide_diff = wide_pos[:, None] - wide_pos[None, :] + (WIN_S - 1)
    return ((time_diff * span_side + high_diff) * span_side + wide_diff).astype(jnp.int32)

def region_labels():
    places = jnp.arange(SIDE, dtype=jnp.int32)
    return (places >= SIDE - WIN_S).astype(jnp.int32) + (places >= SIDE - SHIFT_S).astype(jnp.int32)

def split_windows(grid_field):
    frames = grid_field.shape[0]
    channels = grid_field.shape[-1]
    across = SIDE // WIN_S
    shaped = grid_field.reshape(frames // WIN_T, WIN_T, across, WIN_S, across, WIN_S, channels)
    return shaped.transpose(0, 2, 4, 1, 3, 5, 6).reshape(-1, WIN_ROWS, channels)

def merge_windows(windows, frames):
    channels = windows.shape[-1]
    across = SIDE // WIN_S
    shaped = windows.reshape(frames // WIN_T, across, across, WIN_T, WIN_S, WIN_S, channels)
    return shaped.transpose(0, 3, 1, 4, 2, 5, 6).reshape(frames, SIDE, SIDE, channels)

def window_attention(qkv_block, allowed, bias_heads):
    window_count = qkv_block.shape[0]
    split_parts = qkv_block.reshape(window_count, WIN_ROWS, 3, HEADS, HEAD_DIM)
    queries = split_parts[:, :, 0]
    key_part = split_parts[:, :, 1]
    valued = split_parts[:, :, 2]
    scores = jnp.einsum('bihd,bjhd->bhij', queries, key_part, precision=lax.Precision.HIGHEST) * HEAD_DIM ** (-0.5) + bias_heads[None]
    scores = low_back(scores)
    scores = jnp.where(allowed[:, None], scores, -1e+30)
    row_max = lax.optimization_barrier(jnp.max(scores, axis=-1, keepdims=True))
    exponent = jnp.exp(scores - row_max)
    attn_probs = low(exponent / lax.optimization_barrier(jnp.sum(exponent, axis=-1, keepdims=True)))
    mixed_out = jnp.einsum('bhij,bjhd->bihd', attn_probs, valued, precision=lax.Precision.HIGHEST)
    return mixed_out.reshape(window_count, WIN_ROWS, D)

def attention_branch(block_items, layer_weights, bias_heads):
    token_block, key_block = block_items
    normed = low(layer_norm(token_block, layer_weights[0], layer_weights[1]))
    bias_query = layer_weights[3]
    qkv_bias = jnp.concatenate([bias_query, jnp.zeros_like(bias_query), layer_weights[4]])
    qkv_block = low(low_back(product_high(normed, layer_weights[2]) + qkv_bias))
    allowed = key_block[:, :, None] == key_block[:, None, :]
    mixed_out = low(low_back(window_attention(qkv_block, allowed, bias_heads)))
    return low_back(product_high(mixed_out, layer_weights[6]) + layer_weights[7])

def feed_forward(token_block, layer_weights):
    normed = low(layer_norm(token_block, layer_weights[8], layer_weights[9]))
    hidden = low_back(product_high(normed, layer_weights[10]) + layer_weights[11])
    active = low(jax.nn.gelu(hidden, approximate=False))
    return low_back(product_high(active, layer_weights[12]) + layer_weights[13])

def block_layer(current, clip_row, layer_weights, shifted):
    frames = current.shape[0]
    bias_heads = jnp.transpose(layer_weights[5][relative_index()], (2, 0, 1))
    if shifted:
        moved = jnp.roll(current, (-SHIFT_T, -SHIFT_S, -SHIFT_S), axis=(0, 1, 2))
        moved_ids = jnp.roll(clip_row, -SHIFT_T)
        labels = region_labels()
        key_field = moved_ids[:, None, None] * 9 + labels[None, :, None] * 3 + labels[None, None, :]
    else:
        moved = current
        key_field = jnp.broadcast_to(clip_row[:, None, None], (frames, SIDE, SIDE))
    token_windows = split_windows(moved)
    key_windows = split_windows(key_field[..., None])[..., 0]
    window_count = token_windows.shape[0]
    branch = lax.map(jax.checkpoint(lambda block_items: attention_branch(block_items, layer_weights, bias_heads)), (token_windows.reshape(window_count // 4, 4, WIN_ROWS, D), key_windows.reshape(window_count // 4, 4, WIN_ROWS)))
    branch = merge_windows(branch.reshape(window_count, WIN_ROWS, D), frames)
    if shifted:
        branch = jnp.roll(branch, (SHIFT_T, SHIFT_S, SHIFT_S), axis=(0, 1, 2))
    attended = current + branch
    row_blocks = attended.reshape(frames // (2 * WIN_T), 2 * WIN_T * SIDE * SIDE, D)
    mlp_out = lax.map(jax.checkpoint(lambda token_block: feed_forward(token_block, layer_weights)), row_blocks)
    return attended + mlp_out.reshape(attended.shape)

def reference(inputs, clip_ids, norm1_gain, norm1_bias, qkv_weight, q_bias, v_bias, bias_table, proj_weight, proj_bias, norm2_gain, norm2_bias, fc1_weight, fc1_bias, fc2_weight, fc2_bias, cotangent):
    weights = tuple((member.astype(jnp.float32) for member in (norm1_gain, norm1_bias, qkv_weight, q_bias, v_bias, bias_table, proj_weight, proj_bias, norm2_gain, norm2_bias, fc1_weight, fc1_bias, fc2_weight, fc2_bias)))

    def forward(activations, weight_set):
        results = []
        for group_index in range(activations.shape[0]):
            current = activations[group_index]
            for layer_index in range(LAYERS):
                layer_weights = tuple((member[layer_index] for member in weight_set))
                current = block_layer(current, clip_ids[group_index], layer_weights, layer_index == 1)
            results.append(current)
        return jnp.stack(results)
    outputs, backward = jax.vjp(forward, inputs.astype(jnp.float32), weights)
    input_grad, grads = backward(cotangent.astype(jnp.float32))
    return (outputs.astype(jnp.bfloat16), input_grad.astype(jnp.bfloat16), grads[0], grads[1], grads[2], grads[3], grads[4], grads[5], grads[6], grads[7], grads[8], grads[9], grads[10], grads[11], grads[12], grads[13])
```

```python
from functools import partial
import math

import jax
import jax.numpy as jnp
from jax import lax
from jax.experimental import pallas as pl
from jax.experimental.pallas import tpu as pltpu
from jax.sharding import PartitionSpec as P

D = 512
HEADS = 16
HEAD_DIM = 32
FF = 2048
SIDE = 14
WIN_T = 8
WIN_S = 7
SHIFT_T = 4
SHIFT_S = 3
LAYERS = 2
WIN_ROWS = 392
TABLE_ROWS = 2535
WINDOWS = 4
GROUP = 4
GROUPS = HEADS // GROUP
GW = GROUP * HEAD_DIM
HS = 400
LANES = 1664
OT_LANES = 1792
CODE = 768
BASE = 1536
LOG2E = 1.4426950408889634
QSCALE = HEAD_DIM ** (-0.5) * LOG2E
BIG = 1e30
F32 = jnp.float32
BF16 = jnp.bfloat16
CHUNKS = [(256 * c, 256) for c in range(6)] + [(1536, 128)]


def dot_nn(a, b):
    return lax.dot_general(a, b, (((1,), (0,)), ((), ())), preferred_element_type=F32)


def dot_nt(a, b):
    return lax.dot_general(a, b, (((1,), (1,)), ((), ())), preferred_element_type=F32)


def dot_tn(a, b):
    return lax.dot_general(a, b, (((0,), (0,)), ((), ())), preferred_element_type=F32)


def code_shift(spot):
    return 8 * (84 - (spot // WIN_S * 13 + spot % WIN_S))


def head_lanes(rows):
    return lax.broadcasted_iota(jnp.int32, (rows, GW), 1) // HEAD_DIM


def stack_heads(stack_ref, block):
    lane_head = head_lanes(WIN_ROWS)
    zero = jnp.zeros((), block.dtype)
    for h in range(GROUP):
        stack_ref[HS * h : HS * h + WIN_ROWS, :GW] = jnp.where(lane_head == h, block, zero)


def clear_gaps(stack_ref):
    width = stack_ref.shape[1]
    for h in range(GROUP):
        stop = HS * (h + 1) if h < GROUP - 1 else LANES
        stack_ref[HS * h + 384 : stop, :] = jnp.zeros((stop - HS * h - 384, width), stack_ref.dtype)


def unstack(turned_ref):
    picked = []
    for h in range(GROUP):
        rows = turned_ref[HEAD_DIM * h : HEAD_DIM * (h + 1), 384 * h : 384 * h + 512 + 128]
        if h:
            rows = pltpu.roll(rows, 640 - 16 * h, axis=1)
        picked.append(rows[:, :512])
    return jnp.concatenate(picked, axis=0).T[:WIN_ROWS]


def build_bias(tab_ref, place_ref, bias_ref, rolled):
    bias_ref[0] = jnp.zeros((WIN_ROWS, LANES), F32)
    for h in range(GROUP):
        base = tab_ref[0, h]
        for spot in range(49):
            shift = code_shift(spot)
            rolled[8 * spot : 8 * spot + 8, :] = pltpu.roll(base, BASE - shift, axis=1)[:, :CODE]
        part = dot_nn(rolled[...].astype(BF16), place_ref[h])
        bias_ref[0, :, 384 * h : 384 * h + 512] += part * LOG2E


def forward_kernel(masked, *refs):
    if masked:
        (q_ref, k_ref, v_ref, tab_ref, place_ref, kaug_ref, qaug_ref, o_ref, lse_ref, bias_ref, stack, rolled, turned) = refs
    else:
        (q_ref, k_ref, v_ref, tab_ref, place_ref, o_ref, lse_ref, bias_ref, stack, rolled, turned) = refs

    @pl.when((pl.program_id(0) == 0) & (pl.program_id(1) == 0))
    def _():
        clear_gaps(stack)
        if masked:
            for h in range(GROUP):
                stack[HS * h : HS * h + WIN_ROWS, GW:] = qaug_ref[...]

    @pl.when(pl.program_id(1) == 0)
    def _():
        build_bias(tab_ref, place_ref, bias_ref, rolled)

    stack_heads(stack, q_ref[0])
    keys = k_ref[0]
    if masked:
        keys = jnp.concatenate([keys, kaug_ref[0]], axis=1)
    values = jnp.concatenate([v_ref[0].astype(F32).T, jnp.ones((8, WIN_ROWS), F32)], axis=0).astype(BF16)
    for start, width in CHUNKS:
        scores = dot_nt(keys, stack[start : start + width, :]) + bias_ref[0, :, start : start + width]
        top = jnp.max(scores, axis=0, keepdims=True)
        weights = jnp.exp2(scores - top).astype(BF16)
        mixed = dot_nn(values, weights)
        total = mixed[GW : GW + 1]
        turned[:, start : start + width] = mixed[:GW] * (1.0 / total)
        lse_ref[0, :, start : start + width] = jnp.broadcast_to(top + jnp.log2(total), (8, width))
    o_ref[0] = unstack(turned).astype(BF16)


def backward_kernel(masked, *refs):
    if masked:
        (q_ref, k_ref, v_ref, o_ref, do_ref, lse_ref, bias_ref, place_ref, kaug_ref, qaug_ref,
         dq_ref, dk_ref, dv_ref, dtab_ref, stack, dstack, probs, slopes, turned, bias_sum) = refs
    else:
        (q_ref, k_ref, v_ref, o_ref, do_ref, lse_ref, bias_ref, place_ref,
         dq_ref, dk_ref, dv_ref, dtab_ref, stack, dstack, probs, slopes, turned, bias_sum) = refs

    @pl.when((pl.program_id(0) == 0) & (pl.program_id(1) == 0))
    def _():
        clear_gaps(stack)
        clear_gaps(dstack)
        if masked:
            for h in range(GROUP):
                stack[HS * h : HS * h + WIN_ROWS, GW:] = qaug_ref[...]

    @pl.when(pl.program_id(1) == 0)
    def _():
        bias_sum[...] = jnp.zeros_like(bias_sum)

    stack_heads(stack, q_ref[0])
    stack_heads(dstack, do_ref[0])
    keys = k_ref[0]
    keys_turned = keys.astype(F32).T.astype(BF16)
    if masked:
        keys = jnp.concatenate([keys, kaug_ref[0]], axis=1)
    values = v_ref[0]
    product = do_ref[0].astype(F32) * o_ref[0].astype(F32)
    product = jnp.concatenate([product, jnp.zeros((8, GW), F32)], axis=0)
    product_high = product.astype(BF16)
    product_low = (product - product_high.astype(F32)).astype(BF16)
    head_rows = lax.broadcasted_iota(jnp.int32, (8, GW), 0) == lax.broadcasted_iota(jnp.int32, (8, GW), 1) // HEAD_DIM
    picker = head_rows.astype(F32).astype(BF16)
    deltas = dot_nt(picker, product_high) + dot_nt(picker, product_low)
    delta_row = jnp.concatenate([deltas[h : h + 1] for h in range(GROUP)] + [jnp.zeros((1, LANES - GROUP * HS), F32)], axis=1)
    for start, width in CHUNKS:
        scores = dot_nt(keys, stack[start : start + width, :]) + bias_ref[0, :, start : start + width]
        chances = jnp.exp2(scores - lse_ref[0, :1, start : start + width])
        slope = dot_nt(values, dstack[start : start + width, :])
        slope = chances * (slope - delta_row[:, start : start + width])
        probs[:, start : start + width] = chances.astype(BF16)
        slopes[:, start : start + width] = slope.astype(BF16)
        bias_sum[:, start : start + width] += slope
    dv_ref[0] = dot_nn(probs[...], dstack[...]).astype(BF16)
    dk_ref[0] = (dot_nn(slopes[...], stack[:, :GW]) * math.log(2.0)).astype(BF16)
    for start, width in CHUNKS:
        turned[:, start : start + width] = dot_nn(keys_turned, slopes[:, start : start + width])
    dq_ref[0] = (unstack(turned) * HEAD_DIM ** (-0.5)).astype(BF16)

    @pl.when(pl.program_id(1) == WINDOWS - 1)
    def _():
        dtab_ref[...] = jnp.zeros_like(dtab_ref)
        pad = jnp.zeros((8, BASE - CODE), F32)
        for h in range(GROUP):
            coded = dot_nt(bias_sum[:, 384 * h : 384 * h + 512].astype(BF16), place_ref[h])
            total = jnp.zeros((8, BASE), F32)
            for spot in range(49):
                piece = jnp.concatenate([coded[8 * spot : 8 * spot + 8], pad], axis=1)
                total = total + pltpu.roll(piece, code_shift(spot), axis=1)
            dtab_ref[0, h] = total


def head_block(part):
    return pl.BlockSpec((1, WIN_ROWS, GW), lambda g, w: (w, 0, part * GROUPS + g))


PLAIN = pl.BlockSpec((1, WIN_ROWS, GW), lambda g, w: (w, 0, g))
LSE = pl.BlockSpec((1, 8, LANES), lambda g, w: (g * WINDOWS + w, 0, 0))
BIAS = pl.BlockSpec((1, WIN_ROWS, LANES), lambda g, w: (g, 0, 0))
TABLE = pl.BlockSpec((1, GROUP, 8, BASE), lambda g, w: (g, 0, 0, 0))
PLACE = pl.BlockSpec((GROUP, CODE, 512), lambda g, w: (0, 0, 0), pipeline_mode=pl.Buffered(1))
KAUG = pl.BlockSpec((1, WIN_ROWS, GW), lambda g, w: (w, 0, 0))
QAUG = pl.BlockSpec((WIN_ROWS, GW), lambda g, w: (0, 0))
VMEM_LIMIT = 62 * 1024 * 1024


def attention_forward(qkv, table, place, aug):
    masked = aug is not None
    wide = 2 * GW if masked else GW
    return pl.pallas_call(
        partial(forward_kernel, masked),
        grid=(GROUPS, WINDOWS),
        in_specs=[head_block(0), head_block(1), head_block(2), TABLE, PLACE] + ([KAUG, QAUG] if masked else []),
        out_specs=[PLAIN, LSE, BIAS],
        out_shape=[
            jax.ShapeDtypeStruct((WINDOWS, WIN_ROWS, D), BF16),
            jax.ShapeDtypeStruct((GROUPS * WINDOWS, 8, LANES), F32),
            jax.ShapeDtypeStruct((GROUPS, WIN_ROWS, LANES), F32),
        ],
        scratch_shapes=[
            pltpu.VMEM((LANES, wide), BF16),
            pltpu.VMEM((WIN_ROWS, CODE), F32),
            pltpu.VMEM((GW, OT_LANES), F32),
        ],
        compiler_params=pltpu.CompilerParams(vmem_limit_bytes=VMEM_LIMIT),
        name="attention_forward",
    )(qkv, qkv, qkv, table, place, *(aug or ()))


def attention_backward(qkv, mixed, grad_mixed, lse, bias, place, aug):
    masked = aug is not None
    wide = 2 * GW if masked else GW
    return pl.pallas_call(
        partial(backward_kernel, masked),
        grid=(GROUPS, WINDOWS),
        in_specs=[head_block(0), head_block(1), head_block(2), PLAIN, PLAIN, LSE, BIAS, PLACE] + ([KAUG, QAUG] if masked else []),
        out_specs=[PLAIN, PLAIN, PLAIN, TABLE],
        out_shape=[jax.ShapeDtypeStruct((WINDOWS, WIN_ROWS, D), BF16)] * 3
        + [jax.ShapeDtypeStruct((GROUPS, GROUP, 8, BASE), F32)],
        scratch_shapes=[
            pltpu.VMEM((LANES, wide), BF16),
            pltpu.VMEM((LANES, GW), BF16),
            pltpu.VMEM((WIN_ROWS, LANES), BF16),
            pltpu.VMEM((WIN_ROWS, LANES), BF16),
            pltpu.VMEM((GW, OT_LANES), F32),
            pltpu.VMEM((WIN_ROWS, LANES), F32),
        ],
        compiler_params=pltpu.CompilerParams(vmem_limit_bytes=VMEM_LIMIT),
        name="attention_backward",
    )(qkv, qkv, qkv, mixed, grad_mixed, lse, bias, place, *(aug or ()))


def spread_table(table_rows):
    cube = table_rows.T.reshape(HEADS, 15, 169)
    rows = jnp.stack([cube[:, 7 - tj : 15 - tj] for tj in range(WIN_T)], axis=1)
    rows = rows.transpose(0, 1, 3, 2).reshape(HEADS, WIN_T, 169 * WIN_T)
    rows = jnp.pad(rows, ((0, 0), (0, 0), (0, BASE - 169 * WIN_T)))
    return rows.reshape(GROUPS, GROUP, WIN_T, BASE).astype(F32)


def gather_table(spread):
    rows = spread.reshape(HEADS, WIN_T, BASE)[:, :, : 169 * WIN_T].reshape(HEADS, WIN_T, 169, WIN_T)
    rows = rows.transpose(0, 1, 3, 2)
    total = sum(
        jnp.pad(rows[:, tj], ((0, 0), (7 - tj, tj), (0, 0))) for tj in range(WIN_T)
    )
    return total.reshape(HEADS, TABLE_ROWS).T


def place_codes():
    code = jnp.arange(CODE, dtype=jnp.int32)
    spot_h, spot_w = code // 8 // 13, code // 8 % 13
    lane = (spot_h * WIN_S + spot_w) * 8 + code % 8
    lane = jnp.where((spot_h < WIN_S) & (spot_w < WIN_S), lane, -1000)
    target = lane[None, :] + 16 * jnp.arange(GROUP, dtype=jnp.int32)[:, None]
    return (target[:, :, None] == jnp.arange(512, dtype=jnp.int32)).astype(BF16)


def mask_operands(clip_row, frames):
    index = lax.axis_index("tm")
    wrapped = jnp.concatenate([clip_row, clip_row[:1]])
    own = lax.dynamic_slice_in_dim(wrapped, index * frames + SHIFT_T, 1)
    following = lax.dynamic_slice_in_dim(jnp.concatenate([clip_row, clip_row[:SHIFT_T]]), (index + 1) * frames, 1)
    differs = (own != following).astype(F32)
    token = jnp.arange(WIN_ROWS, dtype=jnp.int32)
    late = (token % 8 >= SHIFT_T).astype(F32)
    low = (token // 8 // WIN_S >= WIN_S - SHIFT_S).astype(F32)
    right = (token // 8 % WIN_S >= WIN_S - SHIFT_S).astype(F32)
    sides = jnp.stack([late, low, right], axis=1)
    window = jnp.arange(WINDOWS)
    weight = jnp.stack(
        [jnp.broadcast_to(differs, (WINDOWS,)), (window // 2).astype(F32), (window % 2).astype(F32)], axis=1
    )
    queries = jnp.concatenate([sides, 1.0 - sides], axis=1)
    keys = -BIG * jnp.concatenate([weight, weight], axis=1)[:, None, :] * jnp.concatenate([1.0 - sides, sides], axis=1)
    queries = jnp.pad(queries, ((0, 0), (0, GW - 6))).astype(BF16)
    keys = jnp.pad(keys, ((0, 0), (0, 0), (0, GW - 6))).astype(BF16)
    return (keys, queries)


def passed_along(value, axis, steps):
    count = lax.axis_size(axis)
    pairs = [(source, (source + steps) % count) for source in range(count)]
    return lax.ppermute(value, axis, pairs)


def to_windows(field):
    channels = field.shape[-1]
    return field.reshape(2, WIN_S, 2, WIN_S, WIN_T, channels).transpose(0, 2, 1, 3, 4, 5).reshape(WINDOWS, WIN_ROWS, channels)


def from_windows(windows):
    channels = windows.shape[-1]
    return windows.reshape(2, 2, WIN_S, WIN_S, WIN_T, channels).transpose(0, 2, 1, 3, 4, 5).reshape(SIDE, SIDE, WIN_T, channels)


def shift_in(field):
    ahead = passed_along(field[:, :, :SHIFT_T], "tm", -1)
    moved = jnp.concatenate([field[:, :, SHIFT_T:], ahead], axis=2)
    return to_windows(jnp.roll(moved, (-SHIFT_S, -SHIFT_S), axis=(0, 1)))


def shift_out(windows):
    moved = jnp.roll(from_windows(windows), (SHIFT_S, SHIFT_S), axis=(0, 1))
    behind = passed_along(moved[:, :, SHIFT_T:], "tm", 1)
    return jnp.concatenate([behind, moved[:, :, :SHIFT_T]], axis=2)


def layer_norm(values, gain_row, shift_row):
    center = values - jnp.mean(values, axis=-1, keepdims=True)
    spread = jnp.mean(center * center, axis=-1, keepdims=True)
    return center * lax.rsqrt(spread + 1e-05) * gain_row + shift_row


def layer_forward(current, layer_weights, place, aug):
    (gain_one, shift_one, weight_qkv, bias_query, bias_value, table_rows, weight_proj, bias_proj,
     gain_two, shift_two, weight_up, bias_up, weight_down, bias_down) = layer_weights
    rows = WINDOWS * WIN_ROWS
    table = spread_table(table_rows)
    normed_one = layer_norm(current, gain_one.astype(F32), shift_one.astype(F32)).astype(BF16)
    qkv_bias = jnp.concatenate([bias_query, jnp.zeros_like(bias_query), bias_value]).astype(F32)
    scales = jnp.concatenate([jnp.full((D,), QSCALE, F32), jnp.ones((2 * D,), F32)])
    qkv = ((dot_nn(normed_one, weight_qkv) + qkv_bias) * scales).astype(BF16).reshape(WINDOWS, WIN_ROWS, 3 * D)
    mixed, lse, bias = attention_forward(qkv, table, place, aug)
    attended = current + dot_nn(mixed.reshape(rows, D), weight_proj) + bias_proj.astype(F32)
    normed_two = layer_norm(attended, gain_two.astype(F32), shift_two.astype(F32)).astype(BF16)
    hidden = dot_nn(normed_two, weight_up) + bias_up.astype(F32)
    active = jax.nn.gelu(hidden, approximate=False).astype(BF16)
    result = attended + dot_nn(active, weight_down) + bias_down.astype(F32)
    return result, (current, normed_one, qkv, mixed, lse, bias, attended, normed_two, hidden, active)


def layer_backward(upstream, saved, layer_weights, place, aug):
    (gain_one, shift_one, weight_qkv, bias_query, bias_value, table_rows, weight_proj, bias_proj,
     gain_two, shift_two, weight_up, bias_up, weight_down, bias_down) = layer_weights
    (current, normed_one, qkv, mixed, lse, bias, attended, normed_two, hidden, active) = saved
    rows = WINDOWS * WIN_ROWS
    grad_out = upstream.astype(BF16)
    grad_down = dot_tn(active, grad_out)
    grad_bias_down = jnp.sum(grad_out, axis=0, dtype=F32)
    grad_active = dot_nt(grad_out, weight_down)
    gelu_back = jax.vjp(partial(jax.nn.gelu, approximate=False), hidden)[1]
    grad_hidden = gelu_back(grad_active)[0].astype(BF16)
    grad_up = dot_tn(normed_two, grad_hidden)
    grad_bias_up = jnp.sum(grad_hidden, axis=0, dtype=F32)
    grad_normed = dot_nt(grad_hidden, weight_up)
    norm_back = jax.vjp(layer_norm, attended, gain_two.astype(F32), shift_two.astype(F32))[1]
    grad_attended, grad_gain_two, grad_shift_two = norm_back(grad_normed)
    grad_attended = grad_attended + upstream
    grad_attn = grad_attended.astype(BF16)
    grad_proj = dot_tn(mixed.reshape(rows, D), grad_attn)
    grad_bias_proj = jnp.sum(grad_attn, axis=0, dtype=F32)
    grad_mixed = dot_nt(grad_attn, weight_proj).astype(BF16).reshape(WINDOWS, WIN_ROWS, D)
    dq, dk, dv, spread = attention_backward(qkv, mixed, grad_mixed, lse, bias, place, aug)
    dq, dk, dv = (part.reshape(rows, D) for part in (dq, dk, dv))
    grad_weight_qkv = jnp.concatenate([dot_tn(normed_one, part) for part in (dq, dk, dv)], axis=1)
    grad_normed = sum(dot_nt(part, weight_qkv[:, i * D : (i + 1) * D]) for i, part in enumerate((dq, dk, dv)))
    norm_back = jax.vjp(layer_norm, current, gain_one.astype(F32), shift_one.astype(F32))[1]
    grad_current, grad_gain_one, grad_shift_one = norm_back(grad_normed)
    layer_grads = (
        grad_gain_one, grad_shift_one, grad_weight_qkv, jnp.sum(dq, axis=0, dtype=F32), jnp.sum(dv, axis=0, dtype=F32),
        gather_table(spread), grad_proj, grad_bias_proj, grad_gain_two, grad_shift_two,
        grad_up, grad_bias_up, grad_down, grad_bias_down,
    )
    return grad_current + grad_attended, layer_grads


def body(inputs, clip_ids, *rest):
    weight_set, cotangent = rest[:-1], rest[-1]
    frames = inputs.shape[1]
    rows = WINDOWS * WIN_ROWS
    place = place_codes()
    aug = mask_operands(clip_ids[0], frames)
    layers = [tuple(member[index] for member in weight_set) for index in range(LAYERS)]
    upstream = shift_in(cotangent[0].transpose(1, 2, 0, 3)).reshape(rows, D).astype(F32)
    current = to_windows(inputs[0].transpose(1, 2, 0, 3)).reshape(rows, D).astype(F32)
    current, saved_first = layer_forward(current, layers[0], place, None)
    current = shift_in(from_windows(current.reshape(WINDOWS, WIN_ROWS, D))).reshape(rows, D)
    current, saved_second = layer_forward(current, layers[1], place, aug)
    block_output = shift_out(current.astype(BF16).reshape(WINDOWS, WIN_ROWS, D)).transpose(2, 0, 1, 3)
    upstream, grads_second = layer_backward(upstream, saved_second, layers[1], place, aug)
    upstream = to_windows(shift_out(upstream.reshape(WINDOWS, WIN_ROWS, D))).reshape(rows, D)
    upstream, grads_first = layer_backward(upstream, saved_first, layers[0], place, None)
    input_grad = from_windows(upstream.astype(BF16).reshape(WINDOWS, WIN_ROWS, D)).transpose(2, 0, 1, 3)
    stacked = [jnp.stack(pair) for pair in zip(grads_first, grads_second)]
    small_places = [0, 1, 3, 4, 5, 7, 8, 9, 11, 13]
    flat_small = jnp.concatenate([stacked[position].reshape(-1) for position in small_places])
    results = [None] * len(weight_set)
    for position in (2, 6, 10, 12):
        shard = lax.psum_scatter(stacked[position], "tm", scatter_dimension=1, tiled=True)
        results[position] = lax.psum(shard.astype(BF16), "dp").astype(F32)
    small_total = lax.psum(flat_small, ("dp", "tm"))
    offset = 0
    for position in small_places:
        member = stacked[position]
        results[position] = small_total[offset : offset + member.size].reshape(member.shape)
        offset = offset + member.size
    return (block_output.reshape(inputs.shape), input_grad.reshape(inputs.shape)) + tuple(results)


def solution(mesh):
    tokens = P("dp", "tm", None, None, None)
    split = P(None, "tm", None)
    placed = (tokens, P("dp", None)) + (P(),) * 14 + (tokens,)
    outs = (tokens, tokens, P(), P(), split, P(), P(), P(), split, P(), P(), P(), split, P(), split, P())
    return jax.shard_map(body, mesh=mesh, in_specs=placed, out_specs=outs, check_vma=False)
```

```python
from functools import partial
import math

import jax
import jax.numpy as jnp
from jax import lax
from jax.experimental import pallas as pl
from jax.experimental.pallas import tpu as pltpu
from jax.sharding import PartitionSpec as P

D = 512
HEADS = 16
HEAD_DIM = 32
FF = 2048
SIDE = 14
WIN_T = 8
WIN_S = 7
SHIFT_T = 4
SHIFT_S = 3
LAYERS = 2
WIN_ROWS = 392
TABLE_ROWS = 2535
WINDOWS = 4
GROUP = 4
GROUPS = HEADS // GROUP
GW = GROUP * HEAD_DIM
HS = 400
LANES = 1664
OT_LANES = 1792
CODE = 768
BASE = 1536
LOG2E = 1.4426950408889634
QSCALE = HEAD_DIM ** (-0.5) * LOG2E
BIG = 1e30
F32 = jnp.float32
BF16 = jnp.bfloat16
CHUNKS = [(256 * c, 256) for c in range(6)] + [(1536, 128)]


def dot_nn(a, b):
    return lax.dot_general(a, b, (((1,), (0,)), ((), ())), preferred_element_type=F32)


def dot_nt(a, b):
    return lax.dot_general(a, b, (((1,), (1,)), ((), ())), preferred_element_type=F32)


def dot_tn(a, b):
    return lax.dot_general(a, b, (((0,), (0,)), ((), ())), preferred_element_type=F32)


def code_shift(spot):
    return 8 * (84 - (spot // WIN_S * 13 + spot % WIN_S))


def head_lanes(rows):
    return lax.broadcasted_iota(jnp.int32, (rows, GW), 1) // HEAD_DIM


def stack_heads(stack_ref, block):
    lane_head = head_lanes(WIN_ROWS)
    zero = jnp.zeros((), block.dtype)
    for h in range(GROUP):
        stack_ref[HS * h : HS * h + WIN_ROWS, :GW] = jnp.where(lane_head == h, block, zero)


def clear_gaps(stack_ref):
    width = stack_ref.shape[1]
    for h in range(GROUP):
        stop = HS * (h + 1) if h < GROUP - 1 else LANES
        stack_ref[HS * h + 384 : stop, :] = jnp.zeros((stop - HS * h - 384, width), stack_ref.dtype)


def unstack(turned_ref):
    picked = []
    for h in range(GROUP):
        rows = turned_ref[HEAD_DIM * h : HEAD_DIM * (h + 1), 384 * h : 384 * h + 512 + 128]
        if h:
            rows = pltpu.roll(rows, 640 - 16 * h, axis=1)
        picked.append(rows[:, :512])
    return jnp.concatenate(picked, axis=0).T[:WIN_ROWS]


def build_bias(tab_ref, place_ref, bias_ref, rolled):
    bias_ref[...] = jnp.zeros((WIN_ROWS, LANES), F32)
    for h in range(GROUP):
        base = tab_ref[0, h]
        for spot in range(49):
            shift = code_shift(spot)
            rolled[8 * spot : 8 * spot + 8, :] = pltpu.roll(base, BASE - shift, axis=1)[:, :CODE]
        part = dot_nn(rolled[...].astype(BF16), place_ref[h])
        bias_ref[:, 384 * h : 384 * h + 512] += part * LOG2E


def forward_kernel(masked, *refs):
    if masked:
        (q_ref, k_ref, v_ref, tab_ref, place_ref, kaug_ref, qaug_ref, o_ref, inv_ref, e_ref, stack, rolled, turned, bias_sum) = refs
    else:
        (q_ref, k_ref, v_ref, tab_ref, place_ref, o_ref, inv_ref, e_ref, stack, rolled, turned, bias_sum) = refs

    @pl.when((pl.program_id(0) == 0) & (pl.program_id(1) == 0))
    def _():
        clear_gaps(stack)
        if masked:
            for h in range(GROUP):
                stack[HS * h : HS * h + WIN_ROWS, GW:] = qaug_ref[...]

    @pl.when(pl.program_id(1) == 0)
    def _():
        build_bias(tab_ref, place_ref, bias_sum, rolled)

    stack_heads(stack, q_ref[0])
    keys = k_ref[0]
    if masked:
        keys = jnp.concatenate([keys, kaug_ref[0]], axis=1)
    values = v_ref[0].astype(F32).T
    values = jnp.concatenate([values, jnp.ones((16, WIN_ROWS), F32)], axis=0).astype(BF16)
    for start, width in CHUNKS:
        scores = dot_nt(keys, stack[start : start + width, :]) + bias_sum[:, start : start + width]
        top = jnp.max(scores, axis=0, keepdims=True)
        e_ref[0, :, start : start + width] = jnp.exp2(scores - top).astype(BF16)
    for start, width in CHUNKS:
        mixed = dot_nn(values, e_ref[0, :, start : start + width])
        inverse = 1.0 / mixed[GW : GW + 8]
        turned[:, start : start + width] = mixed[:GW] * inverse[:1]
        inv_ref[0, :, start : start + width] = inverse
    o_ref[0] = unstack(turned).astype(BF16)


def backward_kernel(q_ref, k_ref, v_ref, do_ref, inv_ref, e_ref, place_ref,
                    dq_ref, dk_ref, dv_ref, dtab_ref, stack, dstack, probs, slopes, turned, bias_sum):
    @pl.when((pl.program_id(0) == 0) & (pl.program_id(1) == 0))
    def _():
        clear_gaps(stack)
        clear_gaps(dstack)

    @pl.when(pl.program_id(1) == 0)
    def _():
        bias_sum[...] = jnp.zeros_like(bias_sum)

    stack_heads(stack, q_ref[0])
    stack_heads(dstack, do_ref[0])
    keys_turned = k_ref[0].astype(F32).T.astype(BF16)
    values = v_ref[0]
    for start, width in CHUNKS:
        lanes = slice(start, start + width)
        chances = e_ref[0, :, lanes].astype(F32) * inv_ref[0, :1, lanes]
        slope = chances * dot_nt(values, dstack[lanes, :])
        slope = slope - chances * jnp.sum(slope, axis=0, keepdims=True)
        probs[:, lanes] = chances.astype(BF16)
        slopes[:, lanes] = slope.astype(BF16)
        bias_sum[:, lanes] += slope
    dv_ref[0] = dot_nn(probs[...], dstack[...]).astype(BF16)
    dk_ref[0] = (dot_nn(slopes[...], stack[...]) * math.log(2.0)).astype(BF16)
    for start, width in CHUNKS:
        turned[:, start : start + width] = dot_nn(keys_turned, slopes[:, start : start + width])
    dq_ref[0] = (unstack(turned) * HEAD_DIM ** (-0.5)).astype(BF16)

    @pl.when(pl.program_id(1) == WINDOWS - 1)
    def _():
        dtab_ref[...] = jnp.zeros_like(dtab_ref)
        pad = jnp.zeros((8, BASE - CODE), F32)
        for h in range(GROUP):
            coded = dot_nt(bias_sum[:, 384 * h : 384 * h + 512].astype(BF16), place_ref[h])
            total = jnp.zeros((8, BASE), F32)
            for spot in range(49):
                piece = jnp.concatenate([coded[8 * spot : 8 * spot + 8], pad], axis=1)
                total = total + pltpu.roll(piece, code_shift(spot), axis=1)
            dtab_ref[0, h] = total


def busy(microseconds):
    return pl.CostEstimate(flops=microseconds * 1_000_000_000, bytes_accessed=microseconds * 1_000_000, transcendentals=0)


def head_block(part):
    return pl.BlockSpec((1, WIN_ROWS, GW), lambda g, w: (w, 0, part * GROUPS + g))


PLAIN = pl.BlockSpec((1, WIN_ROWS, GW), lambda g, w: (w, 0, g))
INV = pl.BlockSpec((1, 8, LANES), lambda g, w: (g * WINDOWS + w, 0, 0))
EXPS = pl.BlockSpec((1, WIN_ROWS, LANES), lambda g, w: (g * WINDOWS + w, 0, 0))
TABLE = pl.BlockSpec((1, GROUP, 8, BASE), lambda g, w: (g, 0, 0, 0))
PLACE = pl.BlockSpec((GROUP, CODE, 512), lambda g, w: (0, 0, 0), pipeline_mode=pl.Buffered(1))
KAUG = pl.BlockSpec((1, WIN_ROWS, GW), lambda g, w: (w, 0, 0))
QAUG = pl.BlockSpec((WIN_ROWS, GW), lambda g, w: (0, 0))
VMEM_LIMIT = 62 * 1024 * 1024


def attention_forward(qkv, table, place, aug):
    masked = aug is not None
    wide = 2 * GW if masked else GW
    return pl.pallas_call(
        partial(forward_kernel, masked),
        grid=(GROUPS, WINDOWS),
        in_specs=[head_block(0), head_block(1), head_block(2), TABLE, PLACE] + ([KAUG, QAUG] if masked else []),
        out_specs=[PLAIN, INV, EXPS],
        out_shape=[
            jax.ShapeDtypeStruct((WINDOWS, WIN_ROWS, D), BF16),
            jax.ShapeDtypeStruct((GROUPS * WINDOWS, 8, LANES), F32),
            jax.ShapeDtypeStruct((GROUPS * WINDOWS, WIN_ROWS, LANES), BF16),
        ],
        scratch_shapes=[
            pltpu.VMEM((LANES, wide), BF16),
            pltpu.VMEM((WIN_ROWS, CODE), F32),
            pltpu.VMEM((GW, OT_LANES), F32),
            pltpu.VMEM((WIN_ROWS, LANES), F32),
        ],
        compiler_params=pltpu.CompilerParams(vmem_limit_bytes=VMEM_LIMIT),
        cost_estimate=busy(31),
        name="attention_forward",
    )(qkv, qkv, qkv, table, place, *(aug or ()))


def attention_backward(qkv, grad_mixed, inverse, exps, place):
    return pl.pallas_call(
        backward_kernel,
        grid=(GROUPS, WINDOWS),
        in_specs=[head_block(0), head_block(1), head_block(2), PLAIN, INV, EXPS, PLACE],
        out_specs=[PLAIN, PLAIN, PLAIN, TABLE],
        out_shape=[jax.ShapeDtypeStruct((WINDOWS, WIN_ROWS, D), BF16)] * 3
        + [jax.ShapeDtypeStruct((GROUPS, GROUP, 8, BASE), F32)],
        scratch_shapes=[
            pltpu.VMEM((LANES, GW), BF16),
            pltpu.VMEM((LANES, GW), BF16),
            pltpu.VMEM((WIN_ROWS, LANES), BF16),
            pltpu.VMEM((WIN_ROWS, LANES), BF16),
            pltpu.VMEM((GW, OT_LANES), F32),
            pltpu.VMEM((WIN_ROWS, LANES), F32),
        ],
        compiler_params=pltpu.CompilerParams(vmem_limit_bytes=VMEM_LIMIT),
        cost_estimate=busy(52),
        name="attention_backward",
    )(qkv, qkv, qkv, grad_mixed, inverse, exps, place)


def spread_table(table_rows):
    cube = table_rows.T.reshape(HEADS, 15, 169)
    rows = jnp.stack([cube[:, 7 - tj : 15 - tj] for tj in range(WIN_T)], axis=1)
    rows = rows.transpose(0, 1, 3, 2).reshape(HEADS, WIN_T, 169 * WIN_T)
    rows = jnp.pad(rows, ((0, 0), (0, 0), (0, BASE - 169 * WIN_T)))
    return rows.reshape(GROUPS, GROUP, WIN_T, BASE).astype(F32)


def gather_table(spread):
    rows = spread.reshape(HEADS, WIN_T, BASE)[:, :, : 169 * WIN_T].reshape(HEADS, WIN_T, 169, WIN_T)
    rows = rows.transpose(0, 1, 3, 2)
    total = sum(
        jnp.pad(rows[:, tj], ((0, 0), (7 - tj, tj), (0, 0))) for tj in range(WIN_T)
    )
    return total.reshape(HEADS, TABLE_ROWS).T


def place_codes():
    code = jnp.arange(CODE, dtype=jnp.int32)
    spot_h, spot_w = code // 8 // 13, code // 8 % 13
    lane = (spot_h * WIN_S + spot_w) * 8 + code % 8
    lane = jnp.where((spot_h < WIN_S) & (spot_w < WIN_S), lane, -1000)
    target = lane[None, :] + 16 * jnp.arange(GROUP, dtype=jnp.int32)[:, None]
    return (target[:, :, None] == jnp.arange(512, dtype=jnp.int32)).astype(BF16)


def mask_operands(clip_row, frames):
    index = lax.axis_index("tm")
    wrapped = jnp.concatenate([clip_row, clip_row[:1]])
    own = lax.dynamic_slice_in_dim(wrapped, index * frames + SHIFT_T, 1)
    following = lax.dynamic_slice_in_dim(jnp.concatenate([clip_row, clip_row[:SHIFT_T]]), (index + 1) * frames, 1)
    differs = (own != following).astype(F32)
    token = jnp.arange(WIN_ROWS, dtype=jnp.int32)
    late = (token % 8 >= SHIFT_T).astype(F32)
    low = (token // 8 // WIN_S >= WIN_S - SHIFT_S).astype(F32)
    right = (token // 8 % WIN_S >= WIN_S - SHIFT_S).astype(F32)
    sides = jnp.stack([late, low, right], axis=1)
    window = jnp.arange(WINDOWS)
    weight = jnp.stack(
        [jnp.broadcast_to(differs, (WINDOWS,)), (window // 2).astype(F32), (window % 2).astype(F32)], axis=1
    )
    queries = jnp.concatenate([sides, 1.0 - sides], axis=1)
    keys = -BIG * jnp.concatenate([weight, weight], axis=1)[:, None, :] * jnp.concatenate([1.0 - sides, sides], axis=1)
    queries = jnp.pad(queries, ((0, 0), (0, GW - 6))).astype(BF16)
    keys = jnp.pad(keys, ((0, 0), (0, 0), (0, GW - 6))).astype(BF16)
    return (keys, queries)


TAIL_SLOPE = 0.21
TAIL_POLY = (
    -0.07194446913289963, 0.2849435841958524, -0.3329670889498132, 0.35241963260033626, -0.09596225895564263,
    0.12572571978855923, 0.06897590427205952, 0.0850992002684089, 0.08370977184002107,
)


def gelu_and_slope(u):
    t = 1.0 / (1.0 + TAIL_SLOPE * jnp.abs(u))
    tail = TAIL_POLY[0] * t + TAIL_POLY[1]
    for coefficient in TAIL_POLY[2:]:
        tail = tail * t + coefficient
    bell = jnp.exp2(u * u * (-0.5 * LOG2E))
    tail = tail * t * bell
    chance = jnp.where(u >= 0.0, 1.0 - tail, tail)
    return u * chance, chance + u * bell * (1.0 / math.sqrt(2.0 * math.pi))


def normalized(values):
    center = values - jnp.mean(values, axis=1, keepdims=True)
    scale = lax.rsqrt(jnp.mean(center * center, axis=1, keepdims=True) + 1e-05)
    return center * scale, scale


def norm_backward(grad_normed, gain, shape, scale):
    e = grad_normed * gain
    return scale * (e - jnp.mean(e, axis=1, keepdims=True) - shape * jnp.mean(e * shape, axis=1, keepdims=True))


def turned_low(block):
    return block.astype(F32).T.astype(BF16)


def column_sum(block):
    return jnp.sum(block, axis=0, keepdims=True)


def project_in_kernel(layer, x_ref, gain_ref, shift_ref, w_ref, qb_ref, vb_ref, n_ref, qkv_ref):
    row = slice(layer, layer + 1)
    shape, _ = normalized(x_ref[0].astype(F32))
    n = (shape * gain_ref[row].astype(F32) + shift_ref[row].astype(F32)).astype(BF16)
    n_ref[0] = n
    qkv_ref[0, :, :D] = ((dot_nn(n, w_ref[0, :, :D]) + qb_ref[row].astype(F32)) * QSCALE).astype(BF16)
    qkv_ref[0, :, D : 2 * D] = dot_nn(n, w_ref[0, :, D : 2 * D]).astype(BF16)
    qkv_ref[0, :, 2 * D :] = (dot_nn(n, w_ref[0, :, 2 * D :]) + vb_ref[row].astype(F32)).astype(BF16)


def feed_forward_kernel(layer, x_ref, o_ref, wp_ref, wu_ref, wd_ref, bp_ref, gain_ref, shift_ref, bu_ref, bd_ref,
                        x1_ref, n_ref, act_ref, slope_ref, x2_ref):
    row = slice(layer, layer + 1)
    x1 = x_ref[0].astype(F32) + dot_nn(o_ref[0], wp_ref[0]) + bp_ref[row].astype(F32)
    x1_ref[0] = x1
    shape, _ = normalized(x1)
    n = (shape * gain_ref[row].astype(F32) + shift_ref[row].astype(F32)).astype(BF16)
    n_ref[0] = n
    total = x1 + bd_ref[row].astype(F32)
    for c in range(4):
        for part in (0, 1):
            cols = slice(512 * c + 256 * part, 512 * c + 256 * part + 256)
            g, slope = gelu_and_slope(dot_nn(n, wu_ref[0, :, cols]) + bu_ref[row, cols].astype(F32))
            act_ref[0, :, cols] = g.astype(BF16)
            slope_ref[0, :, cols] = slope.astype(BF16)
        wide = slice(512 * c, 512 * c + 512)
        total = total + dot_nn(act_ref[0, :, wide], wd_ref[0, wide, :])
    x2_ref[0] = total.astype(x2_ref.dtype)


def feed_backward_kernel(layer, shards, dz_ref, x1_ref, n_ref, o_ref, act_ref, slope_ref, wp_ref, wu_ref, wd_ref, gain_ref,
                         dx1_ref, do_ref, sums_ref, *rest):
    grads, (du, acc_up, acc_down, acc_proj) = rest[:-4], rest[-4:]
    row = slice(layer, layer + 1)
    step = pl.program_id(0)

    @pl.when(step == 0)
    def _():
        sums_ref[...] = jnp.zeros_like(sums_ref)
        acc_up[...] = jnp.zeros_like(acc_up)
        acc_down[...] = jnp.zeros_like(acc_down)
        acc_proj[...] = jnp.zeros_like(acc_proj)

    dz = dz_ref[0].astype(F32)
    dm = dz.astype(BF16)
    dm_turned = turned_low(dm)
    n_turned = turned_low(n_ref[0])
    dn = jnp.zeros((WIN_ROWS, D), F32)
    for c in range(4):
        for part in (0, 1):
            cols = slice(512 * c + 256 * part, 512 * c + 256 * part + 256)
            grad = dot_nt(dm, wd_ref[0, cols, :]) * slope_ref[0, :, cols].astype(F32)
            low = grad.astype(BF16)
            du[:, cols] = low
            sums_ref[0:1, cols] += column_sum(low.astype(F32))
        wide = slice(512 * c, 512 * c + 512)
        acc_down[:, wide] += dot_nn(dm_turned, act_ref[0, :, wide])
        acc_up[:, wide] += dot_nn(n_turned, du[:, wide])
        dn = dn + dot_nt(du[:, wide], wu_ref[0, :, wide])
    shape, scale = normalized(x1_ref[0])
    dx1 = dz + norm_backward(dn, gain_ref[row].astype(F32), shape, scale)
    dx1_ref[0] = dx1
    da = dx1.astype(BF16)
    do_ref[0] = dot_nt(da, wp_ref[0]).astype(BF16)
    acc_proj[...] += dot_nn(turned_low(o_ref[0]), da)
    sums_ref[1:2, :] += jnp.concatenate(
        [column_sum(dm.astype(F32)), column_sum(da.astype(F32)), column_sum(dn * shape), column_sum(dn)], axis=1
    )

    @pl.when(step == WINDOWS - 1)
    def _():
        if shards == 16:
            (packed,) = grads
            for s in range(16):
                for c in range(16):
                    packed[s, 32 * c : 32 * c + 32, :] = acc_up[32 * s : 32 * s + 32, 128 * c : 128 * c + 128].astype(BF16)
                packed[s, 512:1024, :] = acc_down[:, 128 * s : 128 * s + 128].astype(BF16)
                for c in range(4):
                    packed[s, 1024 + 32 * c : 1056 + 32 * c, :] = acc_proj[32 * s : 32 * s + 32, 128 * c : 128 * c + 128].astype(BF16)
        else:
            for target, source in zip(grads, (acc_up, acc_down, acc_proj)):
                target[...] = source[...].astype(BF16)


def project_back_kernel(layer, shards, dq_ref, dk_ref, dv_ref, n_ref, x_ref, dx1_ref, w_ref, gain_ref, dx_ref, sums_ref, grad_ref, acc):
    row = slice(layer, layer + 1)
    step = pl.program_id(0)

    @pl.when(step == 0)
    def _():
        sums_ref[...] = jnp.zeros_like(sums_ref)
        acc[...] = jnp.zeros_like(acc)

    n_turned = turned_low(n_ref[0])
    dn = jnp.zeros((WIN_ROWS, D), F32)
    for i, part in enumerate((dq_ref, dk_ref, dv_ref)):
        cols = slice(D * i, D * i + D)
        dn = dn + dot_nt(part[0], w_ref[0, :, cols])
        acc[:, cols] += dot_nn(n_turned, part[0])
    shape, scale = normalized(x_ref[0].astype(F32))
    dx_ref[0] = (dx1_ref[0] + norm_backward(dn, gain_ref[row].astype(F32), shape, scale)).astype(dx_ref.dtype)
    sums_ref[0:1, :] += jnp.concatenate(
        [column_sum(dq_ref[0].astype(F32)), column_sum(dv_ref[0].astype(F32)), column_sum(dn * shape), column_sum(dn)], axis=1
    )

    @pl.when(step == WINDOWS - 1)
    def _():
        if shards == 16:
            for s in range(16):
                for c in range(12):
                    grad_ref[s, 32 * c : 32 * c + 32, :] = acc[32 * s : 32 * s + 32, 128 * c : 128 * c + 128].astype(BF16)
        else:
            grad_ref[...] = acc[...].astype(BF16)


def window_block(width):
    return pl.BlockSpec((1, WIN_ROWS, width), lambda w: (w, 0, 0))


def window_shape(width, dtype):
    return jax.ShapeDtypeStruct((WINDOWS, WIN_ROWS, width), dtype)


def weight_block(layer, rows, columns):
    return pl.BlockSpec((1, rows, columns), lambda w: (layer, 0, 0), pipeline_mode=pl.Buffered(1))


def whole_block(*shape):
    return pl.BlockSpec(shape, lambda w: (0,) * len(shape))


DENSE_PARAMS = pltpu.CompilerParams(vmem_limit_bytes=VMEM_LIMIT)
ROW = whole_block(LAYERS, D)


def project_in(layer, x, gain, shift, weight, q_bias, v_bias):
    return pl.pallas_call(
        partial(project_in_kernel, layer),
        grid=(WINDOWS,),
        in_specs=[window_block(D), ROW, ROW, weight_block(layer, D, 3 * D), ROW, ROW],
        out_specs=[window_block(D), window_block(3 * D)],
        out_shape=[window_shape(D, BF16), window_shape(3 * D, BF16)],
        compiler_params=DENSE_PARAMS,
        cost_estimate=busy(8),
        name="project_in",
    )(x, gain, shift, weight, q_bias, v_bias)


def feed_forward(layer, x, mixed, wp, wu, wd, bp, gain, shift, bu, bd, out_dtype):
    return pl.pallas_call(
        partial(feed_forward_kernel, layer),
        grid=(WINDOWS,),
        in_specs=[window_block(D), window_block(D), weight_block(layer, D, D), weight_block(layer, D, FF),
                  weight_block(layer, FF, D), ROW, ROW, ROW, whole_block(LAYERS, FF), ROW],
        out_specs=[window_block(D), window_block(D), window_block(FF), window_block(FF), window_block(D)],
        out_shape=[window_shape(D, F32), window_shape(D, BF16), window_shape(FF, BF16), window_shape(FF, BF16),
                   window_shape(D, out_dtype)],
        compiler_params=DENSE_PARAMS,
        cost_estimate=busy(28),
        name="feed_forward",
    )(x, mixed, wp, wu, wd, bp, gain, shift, bu, bd)


def feed_backward(layer, shards, dz, x1, normed, mixed, act, slope, wp, wu, wd, gain):
    if shards == 16:
        grad_shapes = [(16, 1152, 128)]
    else:
        grad_shapes = [(D, FF), (D, FF), (D, D)]
    return pl.pallas_call(
        partial(feed_backward_kernel, layer, shards),
        grid=(WINDOWS,),
        in_specs=[window_block(D), window_block(D), window_block(D), window_block(D), window_block(FF), window_block(FF),
                  weight_block(layer, D, D), weight_block(layer, D, FF), weight_block(layer, FF, D), ROW],
        out_specs=[window_block(D), window_block(D), whole_block(8, FF)] + [whole_block(*shape) for shape in grad_shapes],
        out_shape=[window_shape(D, F32), window_shape(D, BF16), jax.ShapeDtypeStruct((8, FF), F32)]
        + [jax.ShapeDtypeStruct(shape, BF16) for shape in grad_shapes],
        scratch_shapes=[pltpu.VMEM((WIN_ROWS, FF), BF16), pltpu.VMEM((D, FF), F32), pltpu.VMEM((D, FF), F32), pltpu.VMEM((D, D), F32)],
        compiler_params=DENSE_PARAMS,
        cost_estimate=busy(28),
        name="feed_backward",
    )(dz, x1, normed, mixed, act, slope, wp, wu, wd, gain)


def project_back(layer, shards, dq, dk, dv, normed, x, dx1, weight, gain, out_dtype):
    grad_shape = (16, 384, 128) if shards == 16 else (D, 3 * D)
    return pl.pallas_call(
        partial(project_back_kernel, layer, shards),
        grid=(WINDOWS,),
        in_specs=[window_block(D)] * 6 + [weight_block(layer, D, 3 * D), ROW],
        out_specs=[window_block(D), whole_block(8, FF), whole_block(*grad_shape)],
        out_shape=[window_shape(D, out_dtype), jax.ShapeDtypeStruct((8, FF), F32), jax.ShapeDtypeStruct(grad_shape, BF16)],
        scratch_shapes=[pltpu.VMEM((D, 3 * D), F32)],
        compiler_params=DENSE_PARAMS,
        cost_estimate=busy(13),
        name="project_back",
    )(dq, dk, dv, normed, x, dx1, weight, gain)


def passed_along(value, axis, steps):
    count = lax.axis_size(axis)
    pairs = [(source, (source + steps) % count) for source in range(count)]
    return lax.ppermute(value, axis, pairs)


def to_windows(field):
    channels = field.shape[-1]
    return field.reshape(2, WIN_S, 2, WIN_S, WIN_T, channels).transpose(0, 2, 1, 3, 4, 5).reshape(WINDOWS, WIN_ROWS, channels)


def from_windows(windows):
    channels = windows.shape[-1]
    return windows.reshape(2, 2, WIN_S, WIN_S, WIN_T, channels).transpose(0, 2, 1, 3, 4, 5).reshape(SIDE, SIDE, WIN_T, channels)


def shift_in(field):
    ahead = passed_along(field[:, :, :SHIFT_T], "tm", -1)
    moved = jnp.concatenate([field[:, :, SHIFT_T:], ahead], axis=2)
    return to_windows(jnp.roll(moved, (-SHIFT_S, -SHIFT_S), axis=(0, 1)))


def shift_out(windows):
    moved = jnp.roll(from_windows(windows), (SHIFT_S, SHIFT_S), axis=(0, 1))
    behind = passed_along(moved[:, :, SHIFT_T:], "tm", 1)
    return jnp.concatenate([behind, moved[:, :, :SHIFT_T]], axis=2)


def layer_forward(layer, current, weights, place, aug, out_dtype):
    (gain_one, shift_one, weight_qkv, bias_query, bias_value, table_rows, weight_proj, bias_proj,
     gain_two, shift_two, weight_up, bias_up, weight_down, bias_down) = weights
    table = spread_table(table_rows[layer])
    normed_one, qkv = project_in(layer, current, gain_one, shift_one, weight_qkv, bias_query, bias_value)
    mixed, inverse, exps = attention_forward(qkv, table, place, aug)
    attended, normed_two, act, slope, result = feed_forward(
        layer, current, mixed, weight_proj, weight_up, weight_down, bias_proj, gain_two, shift_two, bias_up, bias_down, out_dtype
    )
    return result, (current, normed_one, qkv, mixed, inverse, exps, attended, normed_two, act, slope)


def over_groups(value):
    count = lax.axis_size("dp")
    if count != 2:
        return lax.psum(value, "dp")
    return value.astype(F32) + passed_along(value, "dp", 1).astype(F32)


def scattered(grad):
    shard = lax.psum_scatter(grad, "tm", scatter_dimension=0, tiled=True)
    return over_groups(shard.reshape(shard.shape[-2:])).astype(F32)


def halved(grad):
    count = lax.axis_size("tm")
    index = lax.axis_index("tm")
    kept = grad.reshape((count, -1) + grad.shape[-1:])
    reach = 1
    while reach < count:
        pairs = kept.reshape((kept.shape[0] // 2, 2) + kept.shape[1:])
        bit = index // reach % 2
        mine = lax.dynamic_index_in_dim(pairs, bit, 1, keepdims=False)
        sent = lax.dynamic_index_in_dim(pairs, 1 - bit, 1, keepdims=False).astype(BF16)
        swap = [(source, source ^ reach) for source in range(count)]
        kept = mine.astype(F32) + lax.ppermute(sent, "tm", swap).astype(F32)
        reach = 2 * reach
    return over_groups(kept[0].astype(BF16))


def unpack(packed, start, columns):
    rows = columns // 128 * 32
    return packed[start : start + rows].reshape(columns // 128, 32, 128).transpose(1, 0, 2).reshape(32, columns)


def layer_backward(layer, upstream, saved, weights, place, aug, out_dtype, after):
    (gain_one, shift_one, weight_qkv, bias_query, bias_value, table_rows, weight_proj, bias_proj,
     gain_two, shift_two, weight_up, bias_up, weight_down, bias_down) = weights
    (current, normed_one, qkv, mixed, inverse, exps, attended, normed_two, act, slope) = saved
    shards = lax.axis_size("tm")
    grad_attended, grad_mixed, sums_two, *feed_grads = feed_backward(
        layer, shards, upstream, attended, normed_two, mixed, act, slope, weight_proj, weight_up, weight_down, gain_two
    )
    if shards == 16:
        feed_sums = (scattered(feed_grads[0]),)
    else:
        feed_sums = (scattered(feed_grads[0]), scattered(feed_grads[1].T), scattered(feed_grads[2]))
    dq, dk, dv, spread = attention_backward(qkv, grad_mixed, inverse, exps, place)
    if after is not None:
        dq, after = lax.optimization_barrier((dq, after))
    result, sums_one, grad_qkv = project_back(
        layer, shards, dq, dk, dv, normed_one, current, grad_attended, weight_qkv, gain_one, out_dtype
    )
    grad_qkv = halved(grad_qkv)
    small = jnp.concatenate([sums_two[:2].reshape(-1), sums_one[:1].reshape(-1), gather_table(spread).reshape(-1)])
    if after is not None:
        small, feed_sums = lax.optimization_barrier((small, feed_sums))
    return result, (feed_sums, grad_qkv, lax.psum(small, ("dp", "tm"))), after


def layer_totals(sums):
    feed_sums, grad_qkv, small = sums
    if len(feed_sums) == 1:
        packed = feed_sums[0]
        grad_up = unpack(packed, 0, FF)
        grad_down = packed[512:1024].T
        grad_proj = unpack(packed, 1024, D)
        grad_qkv = unpack(grad_qkv, 0, 3 * D)
    else:
        grad_up, grad_down, grad_proj = feed_sums
    rest = small[FF : 3 * FF].reshape(8, D)
    return (
        rest[6], rest[7], grad_qkv, rest[4], rest[5], small[3 * FF :].reshape(TABLE_ROWS, HEADS), grad_proj, rest[1],
        rest[2], rest[3], grad_up, small[:FF], grad_down, rest[0],
    )


def body(inputs, clip_ids, *rest):
    weights, cotangent = rest[:-1], rest[-1]
    frames = inputs.shape[1]
    place = place_codes()
    aug = mask_operands(clip_ids[0], frames)
    upstream = shift_in(cotangent[0].transpose(1, 2, 0, 3))
    current = to_windows(inputs[0].transpose(1, 2, 0, 3))
    current, saved_first = layer_forward(0, current, weights, place, None, F32)
    current = shift_in(from_windows(current))
    current, saved_second = layer_forward(1, current, weights, place, aug, BF16)
    block_output = shift_out(current).transpose(2, 0, 1, 3)
    upstream, (feed_second, qkv_second, small_second), _ = layer_backward(
        1, upstream, saved_second, weights, place, aug, F32, None
    )
    upstream = to_windows(shift_out(upstream))
    upstream, feed_second = lax.optimization_barrier((upstream, feed_second))
    upstream, first, (qkv_second, small_second) = layer_backward(
        0, upstream, saved_first, weights, place, None, BF16, (qkv_second, small_second)
    )
    totals_first = layer_totals(first)
    totals_second = layer_totals((feed_second, qkv_second, small_second))
    input_grad = from_windows(upstream).transpose(2, 0, 1, 3)
    results = [jnp.stack(pair) for pair in zip(totals_first, totals_second)]
    return (block_output.reshape(inputs.shape), input_grad.reshape(inputs.shape)) + tuple(results)


def solution(mesh):
    tokens = P("dp", "tm", None, None, None)
    split = P(None, "tm", None)
    placed = (tokens, P("dp", None)) + (P(),) * 14 + (tokens,)
    outs = (tokens, tokens, P(), P(), split, P(), P(), P(), split, P(), P(), P(), split, P(), split, P())
    return jax.shard_map(body, mesh=mesh, in_specs=placed, out_specs=outs, check_vma=False)
```

```python
from functools import partial
import math

import jax
import jax.numpy as jnp
from jax import lax
from jax.experimental import pallas as pl
from jax.experimental.pallas import tpu as pltpu
from jax.sharding import PartitionSpec as P


D = 512
HEADS = 16
HEAD_DIM = 32
FF = 2048
SIDE = 14
WIN_T = 8
WIN_S = 7
SHIFT_T = 4
SHIFT_S = 3
LAYERS = 2
WIN_ROWS = 392
TABLE_ROWS = 2535
WINDOWS = 4
GROUP = 4
GROUPS = HEADS // GROUP
GW = GROUP * HEAD_DIM
HS = 400
LANES = 1664
OT_LANES = 1792
CODE = 768
BASE = 1536
LOG2E = 1.4426950408889634
QSCALE = HEAD_DIM ** (-0.5) * LOG2E
BIG = 1e30
F32 = jnp.float32
BF16 = jnp.bfloat16
CHUNKS = [(256 * c, 256) for c in range(6)] + [(1536, 128)]

def dot_nn(a, b):
    return lax.dot_general(a, b, (((1,), (0,)), ((), ())), preferred_element_type=F32)

def dot_nt(a, b):
    return lax.dot_general(a, b, (((1,), (1,)), ((), ())), preferred_element_type=F32)


def code_shift(spot):
    return 8 * (84 - (spot // WIN_S * 13 + spot % WIN_S))

def head_lanes(rows):
    return lax.broadcasted_iota(jnp.int32, (rows, GW), 1) // HEAD_DIM

def stack_heads(stack_ref, block):
    lane_head = head_lanes(WIN_ROWS)
    zero = jnp.zeros((), block.dtype)
    for h in range(GROUP):
        stack_ref[HS * h : HS * h + WIN_ROWS, :GW] = jnp.where(lane_head == h, block, zero)

def clear_gaps(stack_ref):
    width = stack_ref.shape[1]
    for h in range(GROUP):
        stop = HS * (h + 1) if h < GROUP - 1 else LANES
        stack_ref[HS * h + 384 : stop, :] = jnp.zeros((stop - HS * h - 384, width), stack_ref.dtype)

def unstack(turned_ref):
    picked = []
    for h in range(GROUP):
        rows = turned_ref[HEAD_DIM * h : HEAD_DIM * (h + 1), 384 * h : 384 * h + 512 + 128]
        if h:
            rows = pltpu.roll(rows, 640 - 16 * h, axis=1)
        picked.append(rows[:, :512])
    return jnp.concatenate(picked, axis=0).T[:WIN_ROWS]

def build_bias(tab_ref, place_ref, bias_ref, rolled):
    bias_ref[...] = jnp.zeros((WIN_ROWS, LANES), F32)
    for h in range(GROUP):
        base = tab_ref[0, h]
        for spot in range(49):
            shift = code_shift(spot)
            rolled[8 * spot : 8 * spot + 8, :] = pltpu.roll(base, BASE - shift, axis=1)[:, :CODE]
        part = dot_nn(rolled[...].astype(BF16), place_ref[h])
        bias_ref[:, 384 * h : 384 * h + 512] += part * LOG2E

def forward_kernel(masked, *refs):
    if masked:
        (q_ref, k_ref, v_ref, tab_ref, place_ref, kaug_ref, qaug_ref, o_ref, inv_ref, e_ref, stack, rolled, turned, bias_sum) = refs
    else:
        (q_ref, k_ref, v_ref, tab_ref, place_ref, o_ref, inv_ref, e_ref, stack, rolled, turned, bias_sum) = refs

    @pl.when((pl.program_id(0) == 0) & (pl.program_id(1) == 0))
    def _():
        clear_gaps(stack)
        if masked:
            for h in range(GROUP):
                stack[HS * h : HS * h + WIN_ROWS, GW:] = qaug_ref[...]

    @pl.when(pl.program_id(1) == 0)
    def _():
        build_bias(tab_ref, place_ref, bias_sum, rolled)

    stack_heads(stack, q_ref[0])
    keys = k_ref[0]
    if masked:
        keys = jnp.concatenate([keys, kaug_ref[0]], axis=1)
    values = v_ref[0].astype(F32).T
    values = jnp.concatenate([values, jnp.ones((16, WIN_ROWS), F32)], axis=0).astype(BF16)
    for start, width in CHUNKS:
        scores = dot_nt(keys, stack[start : start + width, :]) + bias_sum[:, start : start + width]
        top = jnp.max(scores, axis=0, keepdims=True)
        e_ref[0, :, start : start + width] = jnp.exp2(scores - top).astype(BF16)
    for start, width in CHUNKS:
        mixed = dot_nn(values, e_ref[0, :, start : start + width])
        inverse = 1.0 / mixed[GW : GW + 8]
        turned[:, start : start + width] = mixed[:GW] * inverse[:1]
        inv_ref[0, :, start : start + width] = inverse
    o_ref[0] = unstack(turned).astype(BF16)

def backward_kernel(q_ref, k_ref, v_ref, do_ref, inv_ref, e_ref, place_ref,
                    dq_ref, dk_ref, dv_ref, dtab_ref, stack, dstack, probs, slopes, turned, bias_sum):
    @pl.when((pl.program_id(0) == 0) & (pl.program_id(1) == 0))
    def _():
        clear_gaps(stack)
        clear_gaps(dstack)

    @pl.when(pl.program_id(1) == 0)
    def _():
        bias_sum[...] = jnp.zeros_like(bias_sum)

    stack_heads(stack, q_ref[0])
    stack_heads(dstack, do_ref[0])
    keys_turned = k_ref[0].astype(F32).T.astype(BF16)
    values = v_ref[0]
    for start, width in CHUNKS:
        lanes = slice(start, start + width)
        chances = e_ref[0, :, lanes].astype(F32) * inv_ref[0, :1, lanes]
        slope = chances * dot_nt(values, dstack[lanes, :])
        slope = slope - chances * jnp.sum(slope, axis=0, keepdims=True)
        probs[:, lanes] = chances.astype(BF16)
        slopes[:, lanes] = slope.astype(BF16)
        bias_sum[:, lanes] += slope
    dv_ref[0] = dot_nn(probs[...], dstack[...]).astype(BF16)
    dk_ref[0] = (dot_nn(slopes[...], stack[...]) * math.log(2.0)).astype(BF16)
    for start, width in CHUNKS:
        turned[:, start : start + width] = dot_nn(keys_turned, slopes[:, start : start + width])
    dq_ref[0] = (unstack(turned) * HEAD_DIM ** (-0.5)).astype(BF16)

    @pl.when(pl.program_id(1) == WINDOWS - 1)
    def _():
        dtab_ref[...] = jnp.zeros_like(dtab_ref)
        pad = jnp.zeros((8, BASE - CODE), F32)
        for h in range(GROUP):
            coded = dot_nt(bias_sum[:, 384 * h : 384 * h + 512].astype(BF16), place_ref[h])
            total = jnp.zeros((8, BASE), F32)
            for spot in range(49):
                piece = jnp.concatenate([coded[8 * spot : 8 * spot + 8], pad], axis=1)
                total = total + pltpu.roll(piece, code_shift(spot), axis=1)
            dtab_ref[0, h] = total

def busy(microseconds):
    return pl.CostEstimate(flops=microseconds * 1_000_000_000, bytes_accessed=microseconds * 1_000_000, transcendentals=0)

def head_block(part):
    return pl.BlockSpec((1, WIN_ROWS, GW), lambda g, w: (w, 0, part * GROUPS + g))

PLAIN = pl.BlockSpec((1, WIN_ROWS, GW), lambda g, w: (w, 0, g))
INV = pl.BlockSpec((1, 8, LANES), lambda g, w: (g * WINDOWS + w, 0, 0))
EXPS = pl.BlockSpec((1, WIN_ROWS, LANES), lambda g, w: (g * WINDOWS + w, 0, 0))
TABLE = pl.BlockSpec((1, GROUP, 8, BASE), lambda g, w: (g, 0, 0, 0))
PLACE = pl.BlockSpec((GROUP, CODE, 512), lambda g, w: (0, 0, 0), pipeline_mode=pl.Buffered(1))
KAUG = pl.BlockSpec((1, WIN_ROWS, GW), lambda g, w: (w, 0, 0))
QAUG = pl.BlockSpec((WIN_ROWS, GW), lambda g, w: (0, 0))
VMEM_LIMIT = 62 * 1024 * 1024

def attention_forward(qkv, table, place, aug):
    masked = aug is not None
    wide = 2 * GW if masked else GW
    return pl.pallas_call(
        partial(forward_kernel, masked),
        grid=(GROUPS, WINDOWS),
        in_specs=[head_block(0), head_block(1), head_block(2), TABLE, PLACE] + ([KAUG, QAUG] if masked else []),
        out_specs=[PLAIN, INV, EXPS],
        out_shape=[
            jax.ShapeDtypeStruct((WINDOWS, WIN_ROWS, D), BF16),
            jax.ShapeDtypeStruct((GROUPS * WINDOWS, 8, LANES), F32),
            jax.ShapeDtypeStruct((GROUPS * WINDOWS, WIN_ROWS, LANES), BF16),
        ],
        scratch_shapes=[
            pltpu.VMEM((LANES, wide), BF16),
            pltpu.VMEM((WIN_ROWS, CODE), F32),
            pltpu.VMEM((GW, OT_LANES), F32),
            pltpu.VMEM((WIN_ROWS, LANES), F32),
        ],
        compiler_params=pltpu.CompilerParams(vmem_limit_bytes=VMEM_LIMIT),
        cost_estimate=busy(31),
        name="attention_forward",
    )(qkv, qkv, qkv, table, place, *(aug or ()))

def attention_backward(qkv, grad_mixed, inverse, exps, place):
    return pl.pallas_call(
        backward_kernel,
        grid=(GROUPS, WINDOWS),
        in_specs=[head_block(0), head_block(1), head_block(2), PLAIN, INV, EXPS, PLACE],
        out_specs=[PLAIN, PLAIN, PLAIN, TABLE],
        out_shape=[jax.ShapeDtypeStruct((WINDOWS, WIN_ROWS, D), BF16)] * 3
        + [jax.ShapeDtypeStruct((GROUPS, GROUP, 8, BASE), F32)],
        scratch_shapes=[
            pltpu.VMEM((LANES, GW), BF16),
            pltpu.VMEM((LANES, GW), BF16),
            pltpu.VMEM((WIN_ROWS, LANES), BF16),
            pltpu.VMEM((WIN_ROWS, LANES), BF16),
            pltpu.VMEM((GW, OT_LANES), F32),
            pltpu.VMEM((WIN_ROWS, LANES), F32),
        ],
        compiler_params=pltpu.CompilerParams(vmem_limit_bytes=VMEM_LIMIT),
        cost_estimate=busy(52),
        name="attention_backward",
    )(qkv, qkv, qkv, grad_mixed, inverse, exps, place)


def spread_table(table_rows):
    cube = table_rows.T.reshape(HEADS, 15, 169)
    rows = jnp.stack([cube[:, 7 - tj : 15 - tj] for tj in range(WIN_T)], axis=1)
    rows = rows.transpose(0, 1, 3, 2).reshape(HEADS, WIN_T, 169 * WIN_T)
    rows = jnp.pad(rows, ((0, 0), (0, 0), (0, BASE - 169 * WIN_T)))
    return rows.reshape(GROUPS, GROUP, WIN_T, BASE).astype(F32)

def gather_table(spread):
    rows = spread.reshape(HEADS, WIN_T, BASE)[:, :, : 169 * WIN_T].reshape(HEADS, WIN_T, 169, WIN_T)
    rows = rows.transpose(0, 1, 3, 2)
    total = sum(
        jnp.pad(rows[:, tj], ((0, 0), (7 - tj, tj), (0, 0))) for tj in range(WIN_T)
    )
    return total.reshape(HEADS, TABLE_ROWS).T

def place_codes():
    code = jnp.arange(CODE, dtype=jnp.int32)
    spot_h, spot_w = code // 8 // 13, code // 8 % 13
    lane = (spot_h * WIN_S + spot_w) * 8 + code % 8
    lane = jnp.where((spot_h < WIN_S) & (spot_w < WIN_S), lane, -1000)
    target = lane[None, :] + 16 * jnp.arange(GROUP, dtype=jnp.int32)[:, None]
    return (target[:, :, None] == jnp.arange(512, dtype=jnp.int32)).astype(BF16)

def mask_operands(clip_row, frames):
    index = lax.axis_index("tm")
    wrapped = jnp.concatenate([clip_row, clip_row[:1]])
    own = lax.dynamic_slice_in_dim(wrapped, index * frames + SHIFT_T, 1)
    following = lax.dynamic_slice_in_dim(jnp.concatenate([clip_row, clip_row[:SHIFT_T]]), (index + 1) * frames, 1)
    differs = (own != following).astype(F32)
    token = jnp.arange(WIN_ROWS, dtype=jnp.int32)
    late = (token % 8 >= SHIFT_T).astype(F32)
    low = (token // 8 // WIN_S >= WIN_S - SHIFT_S).astype(F32)
    right = (token // 8 % WIN_S >= WIN_S - SHIFT_S).astype(F32)
    sides = jnp.stack([late, low, right], axis=1)
    window = jnp.arange(WINDOWS)
    weight = jnp.stack(
        [jnp.broadcast_to(differs, (WINDOWS,)), (window // 2).astype(F32), (window % 2).astype(F32)], axis=1
    )
    queries = jnp.concatenate([sides, 1.0 - sides], axis=1)
    keys = -BIG * jnp.concatenate([weight, weight], axis=1)[:, None, :] * jnp.concatenate([1.0 - sides, sides], axis=1)
    queries = jnp.pad(queries, ((0, 0), (0, GW - 6))).astype(BF16)
    keys = jnp.pad(keys, ((0, 0), (0, 0), (0, GW - 6))).astype(BF16)
    return (keys, queries)


TAIL_SLOPE = 0.21
TAIL_POLY = (
    -0.07194446913289963, 0.2849435841958524, -0.3329670889498132, 0.35241963260033626, -0.09596225895564263,
    0.12572571978855923, 0.06897590427205952, 0.0850992002684089, 0.08370977184002107,
)

def gelu_and_slope(u):
    t = 1.0 / (1.0 + TAIL_SLOPE * jnp.abs(u))
    tail = TAIL_POLY[0] * t + TAIL_POLY[1]
    for coefficient in TAIL_POLY[2:]:
        tail = tail * t + coefficient
    bell = jnp.exp2(u * u * (-0.5 * LOG2E))
    tail = tail * t * bell
    chance = jnp.where(u >= 0.0, 1.0 - tail, tail)
    return u * chance, chance + u * bell * (1.0 / math.sqrt(2.0 * math.pi))

def normalized(values):
    center = values - jnp.mean(values, axis=1, keepdims=True)
    scale = lax.rsqrt(jnp.mean(center * center, axis=1, keepdims=True) + 1e-05)
    return center * scale, scale

def norm_backward(grad_normed, gain, shape, scale):
    e = grad_normed * gain
    return scale * (e - jnp.mean(e, axis=1, keepdims=True) - shape * jnp.mean(e * shape, axis=1, keepdims=True))

def turned_low(block):
    return block.astype(F32).T.astype(BF16)

def column_sum(block):
    return jnp.sum(block, axis=0, keepdims=True)

def project_in_kernel(layer, x_ref, gain_ref, shift_ref, w_ref, qb_ref, vb_ref, n_ref, qkv_ref):
    row = slice(layer, layer + 1)
    shape, _ = normalized(x_ref[0].astype(F32))
    n = (shape * gain_ref[row].astype(F32) + shift_ref[row].astype(F32)).astype(BF16)
    n_ref[0] = n
    qkv_ref[0, :, :D] = ((dot_nn(n, w_ref[0, :, :D]) + qb_ref[row].astype(F32)) * QSCALE).astype(BF16)
    qkv_ref[0, :, D : 2 * D] = dot_nn(n, w_ref[0, :, D : 2 * D]).astype(BF16)
    qkv_ref[0, :, 2 * D :] = (dot_nn(n, w_ref[0, :, 2 * D :]) + vb_ref[row].astype(F32)).astype(BF16)

def feed_forward_kernel(layer, x_ref, o_ref, wp_ref, wu_ref, wd_ref, bp_ref, gain_ref, shift_ref, bu_ref, bd_ref,
                        x1_ref, n_ref, act_ref, slope_ref, x2_ref):
    row = slice(layer, layer + 1)
    x1 = x_ref[0].astype(F32) + dot_nn(o_ref[0], wp_ref[0]) + bp_ref[row].astype(F32)
    x1_ref[0] = x1
    shape, _ = normalized(x1)
    n = (shape * gain_ref[row].astype(F32) + shift_ref[row].astype(F32)).astype(BF16)
    n_ref[0] = n
    total = x1 + bd_ref[row].astype(F32)
    for c in range(4):
        for part in (0, 1):
            cols = slice(512 * c + 256 * part, 512 * c + 256 * part + 256)
            g, slope = gelu_and_slope(dot_nn(n, wu_ref[0, :, cols]) + bu_ref[row, cols].astype(F32))
            act_ref[0, :, cols] = g.astype(BF16)
            slope_ref[0, :, cols] = slope.astype(BF16)
        wide = slice(512 * c, 512 * c + 512)
        total = total + dot_nn(act_ref[0, :, wide], wd_ref[0, wide, :])
    x2_ref[0] = total.astype(x2_ref.dtype)

def feed_backward_kernel(layer, shards, dz_ref, x1_ref, n_ref, o_ref, act_ref, slope_ref, wp_ref, wu_ref, wd_ref, gain_ref,
                         dx1_ref, do_ref, sums_ref, *rest):
    grads, (du, acc_up, acc_down, acc_proj) = rest[:-4], rest[-4:]
    row = slice(layer, layer + 1)
    step = pl.program_id(0)

    @pl.when(step == 0)
    def _():
        sums_ref[...] = jnp.zeros_like(sums_ref)
        acc_up[...] = jnp.zeros_like(acc_up)
        acc_down[...] = jnp.zeros_like(acc_down)
        acc_proj[...] = jnp.zeros_like(acc_proj)

    dz = dz_ref[0].astype(F32)
    dm = dz.astype(BF16)
    dm_turned = turned_low(dm)
    n_turned = turned_low(n_ref[0])
    dn = jnp.zeros((WIN_ROWS, D), F32)
    for c in range(4):
        for part in (0, 1):
            cols = slice(512 * c + 256 * part, 512 * c + 256 * part + 256)
            grad = dot_nt(dm, wd_ref[0, cols, :]) * slope_ref[0, :, cols].astype(F32)
            low = grad.astype(BF16)
            du[:, cols] = low
            sums_ref[0:1, cols] += column_sum(low.astype(F32))
        wide = slice(512 * c, 512 * c + 512)
        acc_down[:, wide] += dot_nn(dm_turned, act_ref[0, :, wide])
        acc_up[:, wide] += dot_nn(n_turned, du[:, wide])
        dn = dn + dot_nt(du[:, wide], wu_ref[0, :, wide])
    shape, scale = normalized(x1_ref[0])
    dx1 = dz + norm_backward(dn, gain_ref[row].astype(F32), shape, scale)
    dx1_ref[0] = dx1
    da = dx1.astype(BF16)
    do_ref[0] = dot_nt(da, wp_ref[0]).astype(BF16)
    acc_proj[...] += dot_nn(turned_low(o_ref[0]), da)
    sums_ref[1:2, :] += jnp.concatenate(
        [column_sum(dm.astype(F32)), column_sum(da.astype(F32)), column_sum(dn * shape), column_sum(dn)], axis=1
    )

    @pl.when(step == WINDOWS - 1)
    def _():
        if shards == 16:
            (packed,) = grads
            for s in range(16):
                for c in range(16):
                    packed[s, 32 * c : 32 * c + 32, :] = acc_up[32 * s : 32 * s + 32, 128 * c : 128 * c + 128].astype(BF16)
                packed[s, 512:1024, :] = acc_down[:, 128 * s : 128 * s + 128].astype(BF16)
                for c in range(4):
                    packed[s, 1024 + 32 * c : 1056 + 32 * c, :] = acc_proj[32 * s : 32 * s + 32, 128 * c : 128 * c + 128].astype(BF16)
        else:
            for target, source in zip(grads, (acc_up, acc_down, acc_proj)):
                target[...] = source[...].astype(BF16)

def project_back_kernel(layer, shards, dq_ref, dk_ref, dv_ref, n_ref, x_ref, dx1_ref, w_ref, gain_ref, dx_ref, sums_ref, grad_ref, acc):
    row = slice(layer, layer + 1)
    step = pl.program_id(0)

    @pl.when(step == 0)
    def _():
        sums_ref[...] = jnp.zeros_like(sums_ref)
        acc[...] = jnp.zeros_like(acc)

    n_turned = turned_low(n_ref[0])
    dn = jnp.zeros((WIN_ROWS, D), F32)
    for i, part in enumerate((dq_ref, dk_ref, dv_ref)):
        cols = slice(D * i, D * i + D)
        dn = dn + dot_nt(part[0], w_ref[0, :, cols])
        acc[:, cols] += dot_nn(n_turned, part[0])
    shape, scale = normalized(x_ref[0].astype(F32))
    dx_ref[0] = (dx1_ref[0] + norm_backward(dn, gain_ref[row].astype(F32), shape, scale)).astype(dx_ref.dtype)
    sums_ref[0:1, :] += jnp.concatenate(
        [column_sum(dq_ref[0].astype(F32)), column_sum(dv_ref[0].astype(F32)), column_sum(dn * shape), column_sum(dn)], axis=1
    )

    @pl.when(step == WINDOWS - 1)
    def _():
        if shards == 16:
            for s in range(16):
                for c in range(12):
                    grad_ref[s, 32 * c : 32 * c + 32, :] = acc[32 * s : 32 * s + 32, 128 * c : 128 * c + 128].astype(BF16)
        else:
            grad_ref[...] = acc[...].astype(BF16)

def window_block(width):
    return pl.BlockSpec((1, WIN_ROWS, width), lambda w: (w, 0, 0))

def window_shape(width, dtype):
    return jax.ShapeDtypeStruct((WINDOWS, WIN_ROWS, width), dtype)

def weight_block(layer, rows, columns):
    return pl.BlockSpec((1, rows, columns), lambda w: (layer, 0, 0), pipeline_mode=pl.Buffered(1))

def whole_block(*shape):
    return pl.BlockSpec(shape, lambda w: (0,) * len(shape))

DENSE_PARAMS = pltpu.CompilerParams(vmem_limit_bytes=VMEM_LIMIT)
ROW = whole_block(LAYERS, D)

def project_in(layer, x, gain, shift, weight, q_bias, v_bias):
    return pl.pallas_call(
        partial(project_in_kernel, layer),
        grid=(WINDOWS,),
        in_specs=[window_block(D), ROW, ROW, weight_block(layer, D, 3 * D), ROW, ROW],
        out_specs=[window_block(D), window_block(3 * D)],
        out_shape=[window_shape(D, BF16), window_shape(3 * D, BF16)],
        compiler_params=DENSE_PARAMS,
        cost_estimate=busy(8),
        name="project_in",
    )(x, gain, shift, weight, q_bias, v_bias)

def feed_forward(layer, x, mixed, wp, wu, wd, bp, gain, shift, bu, bd, out_dtype):
    return pl.pallas_call(
        partial(feed_forward_kernel, layer),
        grid=(WINDOWS,),
        in_specs=[window_block(D), window_block(D), weight_block(layer, D, D), weight_block(layer, D, FF),
                  weight_block(layer, FF, D), ROW, ROW, ROW, whole_block(LAYERS, FF), ROW],
        out_specs=[window_block(D), window_block(D), window_block(FF), window_block(FF), window_block(D)],
        out_shape=[window_shape(D, F32), window_shape(D, BF16), window_shape(FF, BF16), window_shape(FF, BF16),
                   window_shape(D, out_dtype)],
        compiler_params=DENSE_PARAMS,
        cost_estimate=busy(28),
        name="feed_forward",
    )(x, mixed, wp, wu, wd, bp, gain, shift, bu, bd)

def feed_backward(layer, shards, dz, x1, normed, mixed, act, slope, wp, wu, wd, gain):
    if shards == 16:
        grad_shapes = [(16, 1152, 128)]
    else:
        grad_shapes = [(D, FF), (D, FF), (D, D)]
    return pl.pallas_call(
        partial(feed_backward_kernel, layer, shards),
        grid=(WINDOWS,),
        in_specs=[window_block(D), window_block(D), window_block(D), window_block(D), window_block(FF), window_block(FF),
                  weight_block(layer, D, D), weight_block(layer, D, FF), weight_block(layer, FF, D), ROW],
        out_specs=[window_block(D), window_block(D), whole_block(8, FF)] + [whole_block(*shape) for shape in grad_shapes],
        out_shape=[window_shape(D, F32), window_shape(D, BF16), jax.ShapeDtypeStruct((8, FF), F32)]
        + [jax.ShapeDtypeStruct(shape, BF16) for shape in grad_shapes],
        scratch_shapes=[pltpu.VMEM((WIN_ROWS, FF), BF16), pltpu.VMEM((D, FF), F32), pltpu.VMEM((D, FF), F32), pltpu.VMEM((D, D), F32)],
        compiler_params=DENSE_PARAMS,
        cost_estimate=busy(28),
        name="feed_backward",
    )(dz, x1, normed, mixed, act, slope, wp, wu, wd, gain)

def project_back(layer, shards, dq, dk, dv, normed, x, dx1, weight, gain, out_dtype):
    grad_shape = (16, 384, 128) if shards == 16 else (D, 3 * D)
    return pl.pallas_call(
        partial(project_back_kernel, layer, shards),
        grid=(WINDOWS,),
        in_specs=[window_block(D)] * 6 + [weight_block(layer, D, 3 * D), ROW],
        out_specs=[window_block(D), whole_block(8, FF), whole_block(*grad_shape)],
        out_shape=[window_shape(D, out_dtype), jax.ShapeDtypeStruct((8, FF), F32), jax.ShapeDtypeStruct(grad_shape, BF16)],
        scratch_shapes=[pltpu.VMEM((D, 3 * D), F32)],
        compiler_params=DENSE_PARAMS,
        cost_estimate=busy(13),
        name="project_back",
    )(dq, dk, dv, normed, x, dx1, weight, gain)


def passed_along(value, axis, steps):
    count = lax.axis_size(axis)
    pairs = [(source, (source + steps) % count) for source in range(count)]
    return lax.ppermute(value, axis, pairs)

def to_windows(field):
    channels = field.shape[-1]
    return field.reshape(2, WIN_S, 2, WIN_S, WIN_T, channels).transpose(0, 2, 1, 3, 4, 5).reshape(WINDOWS, WIN_ROWS, channels)

def from_windows(windows):
    channels = windows.shape[-1]
    return windows.reshape(2, 2, WIN_S, WIN_S, WIN_T, channels).transpose(0, 2, 1, 3, 4, 5).reshape(SIDE, SIDE, WIN_T, channels)

def shift_in(field):
    ahead = passed_along(field[:, :, :SHIFT_T], "tm", -1)
    moved = jnp.concatenate([field[:, :, SHIFT_T:], ahead], axis=2)
    return to_windows(jnp.roll(moved, (-SHIFT_S, -SHIFT_S), axis=(0, 1)))

def shift_out(windows):
    moved = jnp.roll(from_windows(windows), (SHIFT_S, SHIFT_S), axis=(0, 1))
    behind = passed_along(moved[:, :, SHIFT_T:], "tm", 1)
    return jnp.concatenate([behind, moved[:, :, :SHIFT_T]], axis=2)

def layer_forward(layer, current, weights, place, aug, out_dtype):
    (gain_one, shift_one, weight_qkv, bias_query, bias_value, table_rows, weight_proj, bias_proj,
     gain_two, shift_two, weight_up, bias_up, weight_down, bias_down) = weights
    table = spread_table(table_rows[layer])
    normed_one, qkv = project_in(layer, current, gain_one, shift_one, weight_qkv, bias_query, bias_value)
    mixed, inverse, exps = attention_forward(qkv, table, place, aug)
    attended, normed_two, act, slope, result = feed_forward(
        layer, current, mixed, weight_proj, weight_up, weight_down, bias_proj, gain_two, shift_two, bias_up, bias_down, out_dtype
    )
    return result, (current, normed_one, qkv, mixed, inverse, exps, attended, normed_two, act, slope)

def over_groups(value):
    count = lax.axis_size("dp")
    if count != 2:
        return lax.psum(value, "dp")
    return value.astype(F32) + passed_along(value, "dp", 1).astype(F32)

def scattered(grad):
    shard = lax.psum_scatter(grad, "tm", scatter_dimension=0, tiled=True)
    return over_groups(shard.reshape(shard.shape[-2:])).astype(F32)

def swapped(value, reach):
    count = lax.axis_size("tm")
    return lax.ppermute(value, "tm", [(source, source ^ reach) for source in range(count)])

def halved(kept, after):
    count = lax.axis_size("tm")
    index = lax.axis_index("tm")
    reach = 1
    while reach < count:
        pairs = kept.reshape((kept.shape[0] // 2, 2) + kept.shape[1:])
        bit = index // reach % 2
        mine = lax.dynamic_index_in_dim(pairs, bit, 1, keepdims=False)
        sent = lax.dynamic_index_in_dim(pairs, 1 - bit, 1, keepdims=False).astype(BF16)
        kept = mine.astype(F32) + swapped(sent, reach).astype(F32)
        reach = 2 * reach
        if reach == 4:
            kept, after = lax.optimization_barrier((kept, after))
    return over_groups(kept[0].astype(BF16)).astype(F32), after

def gathered(shard):
    index = lax.axis_index("tm")
    whole = shard[None]
    reach = 1
    while reach < lax.axis_size("tm"):
        other = swapped(whole, reach)
        upper = index // reach % 2 == 1
        whole = jnp.concatenate([jnp.where(upper, other, whole), jnp.where(upper, whole, other)], axis=0)
        reach = 2 * reach
    return whole

def reduce_last(qkv_grads, smalls, after):
    count = lax.axis_size("tm")
    flat = jnp.stack(smalls)
    size = flat.shape[1]
    rows = -(-size // (128 * count))
    flat = jnp.pad(flat, ((0, 0), (0, rows * 128 * count - size))).reshape(LAYERS, count, rows, 128)
    parts = [grad.reshape(count, -1, 128) for grad in qkv_grads]
    height = parts[0].shape[1]
    shard, after = halved(jnp.concatenate(parts + [flat[0].astype(BF16), flat[1].astype(BF16)], axis=1), after)
    whole = gathered(shard[LAYERS * height :]).reshape(count, LAYERS, rows * 128)
    whole = whole.transpose(1, 0, 2).reshape(LAYERS, -1)[:, :size]
    qkv = [shard[height * layer : height * (layer + 1)] for layer in range(LAYERS)]
    return qkv, whole, after

def unpack(packed, start, columns):
    rows = columns // 128 * 32
    return packed[start : start + rows].reshape(columns // 128, 32, 128).transpose(1, 0, 2).reshape(32, columns)

def layer_backward(layer, upstream, saved, weights, place, out_dtype):
    (gain_one, _, weight_qkv, _, _, _, weight_proj, _,
     gain_two, _, weight_up, _, weight_down, _) = weights
    (current, normed_one, qkv, mixed, inverse, exps, attended, normed_two, act, slope) = saved
    shards = lax.axis_size("tm")
    grad_attended, grad_mixed, sums_two, *feed_grads = feed_backward(
        layer, shards, upstream, attended, normed_two, mixed, act, slope, weight_proj, weight_up, weight_down, gain_two
    )
    if shards == 16:
        feed_sums = (scattered(feed_grads[0]),)
    else:
        feed_sums = (scattered(feed_grads[0]), scattered(feed_grads[1].T), scattered(feed_grads[2]))
    dq, dk, dv, spread = attention_backward(qkv, grad_mixed, inverse, exps, place)
    result, sums_one, grad_qkv = project_back(
        layer, shards, dq, dk, dv, normed_one, current, grad_attended, weight_qkv, gain_one, out_dtype
    )
    small = jnp.concatenate([sums_two[:2].reshape(-1), sums_one[:1].reshape(-1), gather_table(spread).reshape(-1)])
    return result, feed_sums, grad_qkv, small

def layer_totals(sums):
    feed_sums, grad_qkv, small = sums
    if len(feed_sums) == 1:
        packed = feed_sums[0]
        grad_up = unpack(packed, 0, FF)
        grad_down = packed[512:1024].T
        grad_proj = unpack(packed, 1024, D)
        grad_qkv = unpack(grad_qkv, 0, 3 * D)
    else:
        grad_up, grad_down, grad_proj = feed_sums
        grad_qkv = grad_qkv.reshape(-1, 3 * D)
    rest = small[FF : 3 * FF].reshape(8, D)
    return (
        rest[6], rest[7], grad_qkv, rest[4], rest[5], small[3 * FF :].reshape(TABLE_ROWS, HEADS), grad_proj, rest[1],
        rest[2], rest[3], grad_up, small[:FF], grad_down, rest[0],
    )

def body(inputs, clip_ids, *rest):
    weights, cotangent = rest[:-1], rest[-1]
    frames = inputs.shape[1]
    place = place_codes()
    aug = mask_operands(clip_ids[0], frames)
    upstream = shift_in(cotangent[0].transpose(1, 2, 0, 3))
    current = to_windows(inputs[0].transpose(1, 2, 0, 3))
    current, saved_first = layer_forward(0, current, weights, place, None, F32)
    current = shift_in(from_windows(current))
    current, saved_second = layer_forward(1, current, weights, place, aug, BF16)
    block_output = shift_out(current).transpose(2, 0, 1, 3)
    upstream, feed_second, qkv_second, small_second = layer_backward(1, upstream, saved_second, weights, place, F32)
    upstream = to_windows(shift_out(upstream))

    upstream, feed_first, qkv_first, small_first = layer_backward(0, upstream, saved_first, weights, place, BF16)
    qkv, small, feed_first = reduce_last((qkv_first, qkv_second), (small_first, small_second), feed_first)
    totals_first = layer_totals((feed_first, qkv[0], small[0]))
    totals_second = layer_totals((feed_second, qkv[1], small[1]))
    input_grad = from_windows(upstream).transpose(2, 0, 1, 3)
    results = [jnp.stack(pair) for pair in zip(totals_first, totals_second)]
    return (block_output.reshape(inputs.shape), input_grad.reshape(inputs.shape)) + tuple(results)

def solution(mesh):
    tokens = P("dp", "tm", None, None, None)
    split = P(None, "tm", None)
    placed = (tokens, P("dp", None)) + (P(),) * 14 + (tokens,)
    outs = (tokens, tokens, P(), P(), split, P(), P(), P(), split, P(), P(), P(), split, P(), split, P())
    return jax.shard_map(body, mesh=mesh, in_specs=placed, out_specs=outs, check_vma=False)
```

```python
from functools import partial
import math

import jax
import jax.numpy as jnp
from jax import lax
from jax.experimental import pallas as pl
from jax.experimental.pallas import tpu as pltpu
from jax.sharding import PartitionSpec as P


D = 512
HEADS = 16
HEAD_DIM = 32
FF = 2048
SIDE = 14
WIN_T = 8
WIN_S = 7
SHIFT_T = 4
SHIFT_S = 3
LAYERS = 2
WIN_ROWS = 392
TABLE_ROWS = 2535
WINDOWS = 4
GROUP = 4
GROUPS = HEADS // GROUP
GW = GROUP * HEAD_DIM
HS = 400
LANES = 1664
OT_LANES = 1792
CODE = 768
BASE = 1536
LOG2E = 1.4426950408889634
QSCALE = HEAD_DIM ** (-0.5) * LOG2E
BIG = 1e30
F32 = jnp.float32
BF16 = jnp.bfloat16
CHUNKS = [(256 * c, 256) for c in range(6)] + [(1536, 128)]

def dot_nn(a, b):
    return lax.dot_general(a, b, (((1,), (0,)), ((), ())), preferred_element_type=F32)

def dot_nt(a, b):
    return lax.dot_general(a, b, (((1,), (1,)), ((), ())), preferred_element_type=F32)


def code_shift(spot):
    return 8 * (84 - (spot // WIN_S * 13 + spot % WIN_S))

def head_lanes(rows):
    return lax.broadcasted_iota(jnp.int32, (rows, GW), 1) // HEAD_DIM

def stack_heads(stack_ref, block):
    lane_head = head_lanes(WIN_ROWS)
    zero = jnp.zeros((), block.dtype)
    for h in range(GROUP):
        stack_ref[HS * h : HS * h + WIN_ROWS, :GW] = jnp.where(lane_head == h, block, zero)

def clear_gaps(stack_ref):
    width = stack_ref.shape[1]
    for h in range(GROUP):
        stop = HS * (h + 1) if h < GROUP - 1 else LANES
        stack_ref[HS * h + 384 : stop, :] = jnp.zeros((stop - HS * h - 384, width), stack_ref.dtype)

def unstack(turned_ref):
    picked = []
    for h in range(GROUP):
        rows = turned_ref[HEAD_DIM * h : HEAD_DIM * (h + 1), 384 * h : 384 * h + 512 + 128]
        if h:
            rows = pltpu.roll(rows, 640 - 16 * h, axis=1)
        picked.append(rows[:, :512])
    return jnp.concatenate(picked, axis=0).T[:WIN_ROWS]

def build_bias(tab_ref, place_ref, bias_ref, rolled):
    bias_ref[...] = jnp.zeros((WIN_ROWS, LANES), F32)
    for h in range(GROUP):
        base = tab_ref[0, h]
        for spot in range(49):
            shift = code_shift(spot)
            rolled[8 * spot : 8 * spot + 8, :] = pltpu.roll(base, BASE - shift, axis=1)[:, :CODE]
        part = dot_nn(rolled[...].astype(BF16), place_ref[h])
        bias_ref[:, 384 * h : 384 * h + 512] += part * LOG2E

def forward_kernel(masked, *refs):
    if masked:
        (q_ref, k_ref, v_ref, tab_ref, place_ref, kaug_ref, qaug_ref, o_ref, inv_ref, e_ref, stack, rolled, turned, bias_sum) = refs
    else:
        (q_ref, k_ref, v_ref, tab_ref, place_ref, o_ref, inv_ref, e_ref, stack, rolled, turned, bias_sum) = refs

    @pl.when((pl.program_id(0) == 0) & (pl.program_id(1) == 0))
    def _():
        clear_gaps(stack)
        if masked:
            for h in range(GROUP):
                stack[HS * h : HS * h + WIN_ROWS, GW:] = qaug_ref[...]

    @pl.when(pl.program_id(1) == 0)
    def _():
        build_bias(tab_ref, place_ref, bias_sum, rolled)

    stack_heads(stack, q_ref[0])
    keys = k_ref[0]
    if masked:
        keys = jnp.concatenate([keys, kaug_ref[0]], axis=1)
    values = v_ref[0].astype(F32).T
    values = jnp.concatenate([values, jnp.ones((16, WIN_ROWS), F32)], axis=0).astype(BF16)
    for start, width in CHUNKS:
        scores = dot_nt(keys, stack[start : start + width, :]) + bias_sum[:, start : start + width]
        top = jnp.max(scores, axis=0, keepdims=True)
        e_ref[0, :, start : start + width] = jnp.exp2(scores - top).astype(BF16)
    for start, width in CHUNKS:
        mixed = dot_nn(values, e_ref[0, :, start : start + width])
        inverse = 1.0 / mixed[GW : GW + 8]
        turned[:, start : start + width] = mixed[:GW] * inverse[:1]
        inv_ref[0, :, start : start + width] = inverse
    o_ref[0] = unstack(turned).astype(BF16)

def backward_kernel(q_ref, k_ref, v_ref, do_ref, inv_ref, e_ref, place_ref,
                    dq_ref, dk_ref, dv_ref, dtab_ref, stack, dstack, probs, slopes, turned, bias_sum):
    @pl.when((pl.program_id(0) == 0) & (pl.program_id(1) == 0))
    def _():
        clear_gaps(stack)
        clear_gaps(dstack)

    @pl.when(pl.program_id(1) == 0)
    def _():
        bias_sum[...] = jnp.zeros_like(bias_sum)

    stack_heads(stack, q_ref[0])
    stack_heads(dstack, do_ref[0])
    keys_turned = k_ref[0].astype(F32).T.astype(BF16)
    values = v_ref[0]
    for start, width in CHUNKS:
        lanes = slice(start, start + width)
        chances = e_ref[0, :, lanes].astype(F32) * inv_ref[0, :1, lanes]
        slope = chances * dot_nt(values, dstack[lanes, :])
        slope = slope - chances * jnp.sum(slope, axis=0, keepdims=True)
        probs[:, lanes] = chances.astype(BF16)
        slopes[:, lanes] = slope.astype(BF16)
        bias_sum[:, lanes] += slope
    dv_ref[0] = dot_nn(probs[...], dstack[...]).astype(BF16)
    dk_ref[0] = (dot_nn(slopes[...], stack[...]) * math.log(2.0)).astype(BF16)
    for start, width in CHUNKS:
        turned[:, start : start + width] = dot_nn(keys_turned, slopes[:, start : start + width])
    dq_ref[0] = (unstack(turned) * HEAD_DIM ** (-0.5)).astype(BF16)

    @pl.when(pl.program_id(1) == WINDOWS - 1)
    def _():
        dtab_ref[...] = jnp.zeros_like(dtab_ref)
        pad = jnp.zeros((8, BASE - CODE), F32)
        for h in range(GROUP):
            coded = dot_nt(bias_sum[:, 384 * h : 384 * h + 512].astype(BF16), place_ref[h])
            total = jnp.zeros((8, BASE), F32)
            for spot in range(49):
                piece = jnp.concatenate([coded[8 * spot : 8 * spot + 8], pad], axis=1)
                total = total + pltpu.roll(piece, code_shift(spot), axis=1)
            dtab_ref[0, h] = total

def busy(microseconds):
    return pl.CostEstimate(flops=microseconds * 1_000_000_000, bytes_accessed=microseconds * 1_000_000, transcendentals=0)

def head_block(part):
    return pl.BlockSpec((1, WIN_ROWS, GW), lambda g, w: (w, 0, part * GROUPS + g))

PLAIN = pl.BlockSpec((1, WIN_ROWS, GW), lambda g, w: (w, 0, g))
INV = pl.BlockSpec((1, 8, LANES), lambda g, w: (g * WINDOWS + w, 0, 0))
EXPS = pl.BlockSpec((1, WIN_ROWS, LANES), lambda g, w: (g * WINDOWS + w, 0, 0))
TABLE = pl.BlockSpec((1, GROUP, 8, BASE), lambda g, w: (g, 0, 0, 0))
PLACE = pl.BlockSpec((GROUP, CODE, 512), lambda g, w: (0, 0, 0), pipeline_mode=pl.Buffered(1))
KAUG = pl.BlockSpec((1, WIN_ROWS, GW), lambda g, w: (w, 0, 0))
QAUG = pl.BlockSpec((WIN_ROWS, GW), lambda g, w: (0, 0))
VMEM_LIMIT = 62 * 1024 * 1024

def attention_forward(qkv, table, place, aug):
    masked = aug is not None
    wide = 2 * GW if masked else GW
    return pl.pallas_call(
        partial(forward_kernel, masked),
        grid=(GROUPS, WINDOWS),
        in_specs=[head_block(0), head_block(1), head_block(2), TABLE, PLACE] + ([KAUG, QAUG] if masked else []),
        out_specs=[PLAIN, INV, EXPS],
        out_shape=[
            jax.ShapeDtypeStruct((WINDOWS, WIN_ROWS, D), BF16),
            jax.ShapeDtypeStruct((GROUPS * WINDOWS, 8, LANES), F32),
            jax.ShapeDtypeStruct((GROUPS * WINDOWS, WIN_ROWS, LANES), BF16),
        ],
        scratch_shapes=[
            pltpu.VMEM((LANES, wide), BF16),
            pltpu.VMEM((WIN_ROWS, CODE), F32),
            pltpu.VMEM((GW, OT_LANES), F32),
            pltpu.VMEM((WIN_ROWS, LANES), F32),
        ],
        compiler_params=pltpu.CompilerParams(vmem_limit_bytes=VMEM_LIMIT),
        cost_estimate=busy(31),
        name="attention_forward",
    )(qkv, qkv, qkv, table, place, *(aug or ()))

def attention_backward(qkv, grad_mixed, inverse, exps, place):
    return pl.pallas_call(
        backward_kernel,
        grid=(GROUPS, WINDOWS),
        in_specs=[head_block(0), head_block(1), head_block(2), PLAIN, INV, EXPS, PLACE],
        out_specs=[PLAIN, PLAIN, PLAIN, TABLE],
        out_shape=[jax.ShapeDtypeStruct((WINDOWS, WIN_ROWS, D), BF16)] * 3
        + [jax.ShapeDtypeStruct((GROUPS, GROUP, 8, BASE), F32)],
        scratch_shapes=[
            pltpu.VMEM((LANES, GW), BF16),
            pltpu.VMEM((LANES, GW), BF16),
            pltpu.VMEM((WIN_ROWS, LANES), BF16),
            pltpu.VMEM((WIN_ROWS, LANES), BF16),
            pltpu.VMEM((GW, OT_LANES), F32),
            pltpu.VMEM((WIN_ROWS, LANES), F32),
        ],
        compiler_params=pltpu.CompilerParams(vmem_limit_bytes=VMEM_LIMIT),
        cost_estimate=busy(52),
        name="attention_backward",
    )(qkv, qkv, qkv, grad_mixed, inverse, exps, place)


def spread_table(table_rows):
    cube = table_rows.T.reshape(HEADS, 15, 169)
    rows = jnp.stack([cube[:, 7 - tj : 15 - tj] for tj in range(WIN_T)], axis=1)
    rows = rows.transpose(0, 1, 3, 2).reshape(HEADS, WIN_T, 169 * WIN_T)
    rows = jnp.pad(rows, ((0, 0), (0, 0), (0, BASE - 169 * WIN_T)))
    return rows.reshape(GROUPS, GROUP, WIN_T, BASE).astype(F32)

def gather_table(spread):
    rows = spread.reshape(HEADS, WIN_T, BASE)[:, :, : 169 * WIN_T].reshape(HEADS, WIN_T, 169, WIN_T)
    rows = rows.transpose(0, 1, 3, 2)
    total = sum(
        jnp.pad(rows[:, tj], ((0, 0), (7 - tj, tj), (0, 0))) for tj in range(WIN_T)
    )
    return total.reshape(HEADS, TABLE_ROWS).T

def place_codes():
    code = jnp.arange(CODE, dtype=jnp.int32)
    spot_h, spot_w = code // 8 // 13, code // 8 % 13
    lane = (spot_h * WIN_S + spot_w) * 8 + code % 8
    lane = jnp.where((spot_h < WIN_S) & (spot_w < WIN_S), lane, -1000)
    target = lane[None, :] + 16 * jnp.arange(GROUP, dtype=jnp.int32)[:, None]
    return (target[:, :, None] == jnp.arange(512, dtype=jnp.int32)).astype(BF16)

def mask_operands(clip_row, frames):
    index = lax.axis_index("tm")
    wrapped = jnp.concatenate([clip_row, clip_row[:1]])
    own = lax.dynamic_slice_in_dim(wrapped, index * frames + SHIFT_T, 1)
    following = lax.dynamic_slice_in_dim(jnp.concatenate([clip_row, clip_row[:SHIFT_T]]), (index + 1) * frames, 1)
    differs = (own != following).astype(F32)
    token = jnp.arange(WIN_ROWS, dtype=jnp.int32)
    late = (token % 8 >= SHIFT_T).astype(F32)
    low = (token // 8 // WIN_S >= WIN_S - SHIFT_S).astype(F32)
    right = (token // 8 % WIN_S >= WIN_S - SHIFT_S).astype(F32)
    sides = jnp.stack([late, low, right], axis=1)
    window = jnp.arange(WINDOWS)
    weight = jnp.stack(
        [jnp.broadcast_to(differs, (WINDOWS,)), (window // 2).astype(F32), (window % 2).astype(F32)], axis=1
    )
    queries = jnp.concatenate([sides, 1.0 - sides], axis=1)
    keys = -BIG * jnp.concatenate([weight, weight], axis=1)[:, None, :] * jnp.concatenate([1.0 - sides, sides], axis=1)
    queries = jnp.pad(queries, ((0, 0), (0, GW - 6))).astype(BF16)
    keys = jnp.pad(keys, ((0, 0), (0, 0), (0, GW - 6))).astype(BF16)
    return (keys, queries)


TAIL_SLOPE = 0.21
TAIL_POLY = (
    -0.07194446913289963, 0.2849435841958524, -0.3329670889498132, 0.35241963260033626, -0.09596225895564263,
    0.12572571978855923, 0.06897590427205952, 0.0850992002684089, 0.08370977184002107,
)

def gelu_and_slope(u):
    t = 1.0 / (1.0 + TAIL_SLOPE * jnp.abs(u))
    tail = TAIL_POLY[0] * t + TAIL_POLY[1]
    for coefficient in TAIL_POLY[2:]:
        tail = tail * t + coefficient
    bell = jnp.exp2(u * u * (-0.5 * LOG2E))
    tail = tail * t * bell
    chance = jnp.where(u >= 0.0, 1.0 - tail, tail)
    return u * chance, chance + u * bell * (1.0 / math.sqrt(2.0 * math.pi))

def normalized(values):
    center = values - jnp.mean(values, axis=1, keepdims=True)
    scale = lax.rsqrt(jnp.mean(center * center, axis=1, keepdims=True) + 1e-05)
    return center * scale, scale

def norm_backward(grad_normed, gain, shape, scale):
    e = grad_normed * gain
    return scale * (e - jnp.mean(e, axis=1, keepdims=True) - shape * jnp.mean(e * shape, axis=1, keepdims=True))

def turned_low(block):
    return block.astype(F32).T.astype(BF16)

def column_sum(block):
    return jnp.sum(block, axis=0, keepdims=True)

def project_in_kernel(layer, x_ref, gain_ref, shift_ref, w_ref, qb_ref, vb_ref, n_ref, qkv_ref):
    row = slice(layer, layer + 1)
    shape, _ = normalized(x_ref[0].astype(F32))
    n = (shape * gain_ref[row].astype(F32) + shift_ref[row].astype(F32)).astype(BF16)
    n_ref[0] = n
    qkv_ref[0, :, :D] = ((dot_nn(n, w_ref[0, :, :D]) + qb_ref[row].astype(F32)) * QSCALE).astype(BF16)
    qkv_ref[0, :, D : 2 * D] = dot_nn(n, w_ref[0, :, D : 2 * D]).astype(BF16)
    qkv_ref[0, :, 2 * D :] = (dot_nn(n, w_ref[0, :, 2 * D :]) + vb_ref[row].astype(F32)).astype(BF16)

def feed_forward_kernel(layer, x_ref, o_ref, wp_ref, wu_ref, wd_ref, bp_ref, gain_ref, shift_ref, bu_ref, bd_ref,
                        x1_ref, n_ref, act_ref, slope_ref, x2_ref):
    row = slice(layer, layer + 1)
    x1 = x_ref[0].astype(F32) + dot_nn(o_ref[0], wp_ref[0]) + bp_ref[row].astype(F32)
    x1_ref[0] = x1
    shape, _ = normalized(x1)
    n = (shape * gain_ref[row].astype(F32) + shift_ref[row].astype(F32)).astype(BF16)
    n_ref[0] = n
    total = x1 + bd_ref[row].astype(F32)
    for c in range(4):
        for part in (0, 1):
            cols = slice(512 * c + 256 * part, 512 * c + 256 * part + 256)
            g, slope = gelu_and_slope(dot_nn(n, wu_ref[0, :, cols]) + bu_ref[row, cols].astype(F32))
            act_ref[0, :, cols] = g.astype(BF16)
            slope_ref[0, :, cols] = slope.astype(BF16)
        wide = slice(512 * c, 512 * c + 512)
        total = total + dot_nn(act_ref[0, :, wide], wd_ref[0, wide, :])
    x2_ref[0] = total.astype(x2_ref.dtype)

def feed_backward_kernel(layer, shards, dz_ref, x1_ref, n_ref, o_ref, act_ref, slope_ref, wp_ref, wu_ref, wd_ref, gain_ref,
                         dx1_ref, do_ref, sums_ref, *rest):
    grads, (du, acc_up, acc_down, acc_proj) = rest[:-4], rest[-4:]
    row = slice(layer, layer + 1)
    step = pl.program_id(0)

    @pl.when(step == 0)
    def _():
        sums_ref[...] = jnp.zeros_like(sums_ref)
        acc_up[...] = jnp.zeros_like(acc_up)
        acc_down[...] = jnp.zeros_like(acc_down)
        acc_proj[...] = jnp.zeros_like(acc_proj)

    dz = dz_ref[0].astype(F32)
    dm = dz.astype(BF16)
    dm_turned = turned_low(dm)
    n_turned = turned_low(n_ref[0])
    dn = jnp.zeros((WIN_ROWS, D), F32)
    for c in range(4):
        for part in (0, 1):
            cols = slice(512 * c + 256 * part, 512 * c + 256 * part + 256)
            grad = dot_nt(dm, wd_ref[0, cols, :]) * slope_ref[0, :, cols].astype(F32)
            low = grad.astype(BF16)
            du[:, cols] = low
            sums_ref[0:1, cols] += column_sum(low.astype(F32))
        wide = slice(512 * c, 512 * c + 512)
        acc_down[:, wide] += dot_nn(dm_turned, act_ref[0, :, wide])
        acc_up[:, wide] += dot_nn(n_turned, du[:, wide])
        dn = dn + dot_nt(du[:, wide], wu_ref[0, :, wide])
    shape, scale = normalized(x1_ref[0])
    dx1 = dz + norm_backward(dn, gain_ref[row].astype(F32), shape, scale)
    dx1_ref[0] = dx1
    da = dx1.astype(BF16)
    do_ref[0] = dot_nt(da, wp_ref[0]).astype(BF16)
    acc_proj[...] += dot_nn(turned_low(o_ref[0]), da)
    sums_ref[1:2, :] += jnp.concatenate(
        [column_sum(dm.astype(F32)), column_sum(da.astype(F32)), column_sum(dn * shape), column_sum(dn)], axis=1
    )

    @pl.when(step == WINDOWS - 1)
    def _():
        if shards == 16:
            (packed,) = grads
            for s in range(16):
                for c in range(16):
                    packed[s, 32 * c : 32 * c + 32, :] = acc_up[32 * s : 32 * s + 32, 128 * c : 128 * c + 128].astype(BF16)
                packed[s, 512:1024, :] = acc_down[:, 128 * s : 128 * s + 128].astype(BF16)
                for c in range(4):
                    packed[s, 1024 + 32 * c : 1056 + 32 * c, :] = acc_proj[32 * s : 32 * s + 32, 128 * c : 128 * c + 128].astype(BF16)
        else:
            for target, source in zip(grads, (acc_up, acc_down, acc_proj)):
                target[...] = source[...].astype(BF16)

def project_back_kernel(layer, shards, dq_ref, dk_ref, dv_ref, n_ref, x_ref, dx1_ref, w_ref, gain_ref, dx_ref, sums_ref, grad_ref, acc):
    row = slice(layer, layer + 1)
    step = pl.program_id(0)

    @pl.when(step == 0)
    def _():
        sums_ref[...] = jnp.zeros_like(sums_ref)
        acc[...] = jnp.zeros_like(acc)

    n_turned = turned_low(n_ref[0])
    dn = jnp.zeros((WIN_ROWS, D), F32)
    for i, part in enumerate((dq_ref, dk_ref, dv_ref)):
        cols = slice(D * i, D * i + D)
        dn = dn + dot_nt(part[0], w_ref[0, :, cols])
        acc[:, cols] += dot_nn(n_turned, part[0])
    shape, scale = normalized(x_ref[0].astype(F32))
    dx_ref[0] = (dx1_ref[0] + norm_backward(dn, gain_ref[row].astype(F32), shape, scale)).astype(dx_ref.dtype)
    sums_ref[0:1, :] += jnp.concatenate(
        [column_sum(dq_ref[0].astype(F32)), column_sum(dv_ref[0].astype(F32)), column_sum(dn * shape), column_sum(dn)], axis=1
    )

    @pl.when(step == WINDOWS - 1)
    def _():
        if shards == 16:
            for s in range(16):
                for c in range(12):
                    grad_ref[s, 32 * c : 32 * c + 32, :] = acc[32 * s : 32 * s + 32, 128 * c : 128 * c + 128].astype(BF16)
        else:
            grad_ref[...] = acc[...].astype(BF16)

def window_block(width):
    return pl.BlockSpec((1, WIN_ROWS, width), lambda w: (w, 0, 0))

def window_shape(width, dtype):
    return jax.ShapeDtypeStruct((WINDOWS, WIN_ROWS, width), dtype)

def weight_block(layer, rows, columns):
    return pl.BlockSpec((1, rows, columns), lambda w: (layer, 0, 0), pipeline_mode=pl.Buffered(1))

def whole_block(*shape):
    return pl.BlockSpec(shape, lambda w: (0,) * len(shape))

DENSE_PARAMS = pltpu.CompilerParams(vmem_limit_bytes=VMEM_LIMIT)
ROW = whole_block(LAYERS, D)

def project_in(layer, x, gain, shift, weight, q_bias, v_bias):
    return pl.pallas_call(
        partial(project_in_kernel, layer),
        grid=(WINDOWS,),
        in_specs=[window_block(D), ROW, ROW, weight_block(layer, D, 3 * D), ROW, ROW],
        out_specs=[window_block(D), window_block(3 * D)],
        out_shape=[window_shape(D, BF16), window_shape(3 * D, BF16)],
        compiler_params=DENSE_PARAMS,
        cost_estimate=busy(8),
        name="project_in",
    )(x, gain, shift, weight, q_bias, v_bias)

def feed_forward(layer, x, mixed, wp, wu, wd, bp, gain, shift, bu, bd, out_dtype):
    return pl.pallas_call(
        partial(feed_forward_kernel, layer),
        grid=(WINDOWS,),
        in_specs=[window_block(D), window_block(D), weight_block(layer, D, D), weight_block(layer, D, FF),
                  weight_block(layer, FF, D), ROW, ROW, ROW, whole_block(LAYERS, FF), ROW],
        out_specs=[window_block(D), window_block(D), window_block(FF), window_block(FF), window_block(D)],
        out_shape=[window_shape(D, F32), window_shape(D, BF16), window_shape(FF, BF16), window_shape(FF, BF16),
                   window_shape(D, out_dtype)],
        compiler_params=DENSE_PARAMS,
        cost_estimate=busy(28),
        name="feed_forward",
    )(x, mixed, wp, wu, wd, bp, gain, shift, bu, bd)

def feed_backward(layer, shards, dz, x1, normed, mixed, act, slope, wp, wu, wd, gain):
    if shards == 16:
        grad_shapes = [(16, 1152, 128)]
    else:
        grad_shapes = [(D, FF), (D, FF), (D, D)]
    return pl.pallas_call(
        partial(feed_backward_kernel, layer, shards),
        grid=(WINDOWS,),
        in_specs=[window_block(D), window_block(D), window_block(D), window_block(D), window_block(FF), window_block(FF),
                  weight_block(layer, D, D), weight_block(layer, D, FF), weight_block(layer, FF, D), ROW],
        out_specs=[window_block(D), window_block(D), whole_block(8, FF)] + [whole_block(*shape) for shape in grad_shapes],
        out_shape=[window_shape(D, F32), window_shape(D, BF16), jax.ShapeDtypeStruct((8, FF), F32)]
        + [jax.ShapeDtypeStruct(shape, BF16) for shape in grad_shapes],
        scratch_shapes=[pltpu.VMEM((WIN_ROWS, FF), BF16), pltpu.VMEM((D, FF), F32), pltpu.VMEM((D, FF), F32), pltpu.VMEM((D, D), F32)],
        compiler_params=DENSE_PARAMS,
        cost_estimate=busy(28),
        name="feed_backward",
    )(dz, x1, normed, mixed, act, slope, wp, wu, wd, gain)

def project_back(layer, shards, dq, dk, dv, normed, x, dx1, weight, gain, out_dtype):
    grad_shape = (16, 384, 128) if shards == 16 else (D, 3 * D)
    return pl.pallas_call(
        partial(project_back_kernel, layer, shards),
        grid=(WINDOWS,),
        in_specs=[window_block(D)] * 6 + [weight_block(layer, D, 3 * D), ROW],
        out_specs=[window_block(D), whole_block(8, FF), whole_block(*grad_shape)],
        out_shape=[window_shape(D, out_dtype), jax.ShapeDtypeStruct((8, FF), F32), jax.ShapeDtypeStruct(grad_shape, BF16)],
        scratch_shapes=[pltpu.VMEM((D, 3 * D), F32)],
        compiler_params=DENSE_PARAMS,
        cost_estimate=busy(13),
        name="project_back",
    )(dq, dk, dv, normed, x, dx1, weight, gain)


def passed_along(value, axis, steps):
    count = lax.axis_size(axis)
    pairs = [(source, (source + steps) % count) for source in range(count)]
    return lax.ppermute(value, axis, pairs)

def to_windows(field):
    channels = field.shape[-1]
    return field.reshape(2, WIN_S, 2, WIN_S, WIN_T, channels).transpose(0, 2, 1, 3, 4, 5).reshape(WINDOWS, WIN_ROWS, channels)

def from_windows(windows):
    channels = windows.shape[-1]
    return windows.reshape(2, 2, WIN_S, WIN_S, WIN_T, channels).transpose(0, 2, 1, 3, 4, 5).reshape(SIDE, SIDE, WIN_T, channels)

def shift_in(field):
    ahead = passed_along(field[:, :, :SHIFT_T].astype(BF16), "tm", -1).astype(field.dtype)
    moved = jnp.concatenate([field[:, :, SHIFT_T:], ahead], axis=2)
    return to_windows(jnp.roll(moved, (-SHIFT_S, -SHIFT_S), axis=(0, 1)))

def shift_out(windows):
    moved = jnp.roll(from_windows(windows), (SHIFT_S, SHIFT_S), axis=(0, 1))
    behind = passed_along(moved[:, :, SHIFT_T:].astype(BF16), "tm", 1).astype(moved.dtype)
    return jnp.concatenate([behind, moved[:, :, :SHIFT_T]], axis=2)

def layer_forward(layer, current, weights, place, aug, out_dtype):
    (gain_one, shift_one, weight_qkv, bias_query, bias_value, table_rows, weight_proj, bias_proj,
     gain_two, shift_two, weight_up, bias_up, weight_down, bias_down) = weights
    table = spread_table(table_rows[layer])
    normed_one, qkv = project_in(layer, current, gain_one, shift_one, weight_qkv, bias_query, bias_value)
    mixed, inverse, exps = attention_forward(qkv, table, place, aug)
    attended, normed_two, act, slope, result = feed_forward(
        layer, current, mixed, weight_proj, weight_up, weight_down, bias_proj, gain_two, shift_two, bias_up, bias_down, out_dtype
    )
    return result, (current, normed_one, qkv, mixed, inverse, exps, attended, normed_two, act, slope)

def over_groups(value):
    count = lax.axis_size("dp")
    if count != 2:
        return lax.psum(value, "dp")
    return value.astype(F32) + passed_along(value, "dp", 1).astype(F32)

def scattered(grad):
    shard = lax.psum_scatter(grad, "tm", scatter_dimension=0, tiled=True)
    return over_groups(shard.reshape(shard.shape[-2:])).astype(F32)

def swapped(value, reach):
    count = lax.axis_size("tm")
    return lax.ppermute(value, "tm", [(source, source ^ reach) for source in range(count)])

def halved(kept, after):
    count = lax.axis_size("tm")
    index = lax.axis_index("tm")
    reach = 1
    while reach < count:
        pairs = kept.reshape((kept.shape[0] // 2, 2) + kept.shape[1:])
        bit = index // reach % 2
        mine = lax.dynamic_index_in_dim(pairs, bit, 1, keepdims=False)
        sent = lax.dynamic_index_in_dim(pairs, 1 - bit, 1, keepdims=False).astype(BF16)
        kept = mine.astype(F32) + swapped(sent, reach).astype(F32)
        reach = 2 * reach
        if reach == 4:
            kept, after = lax.optimization_barrier((kept, after))
    return over_groups(kept[0].astype(BF16)).astype(F32), after

def gathered(shard):
    count = lax.axis_size("tm")
    index = lax.axis_index("tm")
    whole = shard[None]
    reach = 1
    while reach < count:
        low = index // reach % 2 == 1
        if count // reach >= 4:
            high = index // (2 * reach) % 2 == 1
            one, two, three = (swapped(whole, reach * step) for step in (1, 2, 3))
            first, second = jnp.where(low, one, whole), jnp.where(low, whole, one)
            third, fourth = jnp.where(low, three, two), jnp.where(low, two, three)
            whole = jnp.concatenate(
                [jnp.where(high, third, first), jnp.where(high, fourth, second),
                 jnp.where(high, first, third), jnp.where(high, second, fourth)], axis=0
            )
            reach = 4 * reach
        else:
            other = swapped(whole, reach)
            whole = jnp.concatenate([jnp.where(low, other, whole), jnp.where(low, whole, other)], axis=0)
            reach = 2 * reach
    return whole


def reduce_last(qkv_grads, smalls, after):
    count = lax.axis_size("tm")
    flat = jnp.stack(smalls)
    size = flat.shape[1]
    rows = -(-size // (128 * count))
    flat = jnp.pad(flat, ((0, 0), (0, rows * 128 * count - size))).reshape(LAYERS, count, rows, 128)
    parts = [grad.reshape(count, -1, 128) for grad in qkv_grads]
    height = parts[0].shape[1]
    shard, after = halved(jnp.concatenate(parts + [flat[0].astype(BF16), flat[1].astype(BF16)], axis=1), after)
    whole = gathered(shard[LAYERS * height :]).reshape(count, LAYERS, rows * 128)
    whole = whole.transpose(1, 0, 2).reshape(LAYERS, -1)[:, :size]
    qkv = [shard[height * layer : height * (layer + 1)] for layer in range(LAYERS)]
    return qkv, whole, after

def unpack(packed, start, columns):
    rows = columns // 128 * 32
    return packed[start : start + rows].reshape(columns // 128, 32, 128).transpose(1, 0, 2).reshape(32, columns)

def layer_backward(layer, upstream, saved, weights, place, out_dtype, after):
    (gain_one, _, weight_qkv, _, _, _, weight_proj, _,
     gain_two, _, weight_up, _, weight_down, _) = weights
    (current, normed_one, qkv, mixed, inverse, exps, attended, normed_two, act, slope) = saved
    shards = lax.axis_size("tm")
    grad_attended, grad_mixed, sums_two, *feed_grads = feed_backward(
        layer, shards, upstream, attended, normed_two, mixed, act, slope, weight_proj, weight_up, weight_down, gain_two
    )
    if shards == 16:
        feed_sums = (scattered(feed_grads[0]),)
    else:
        feed_sums = (scattered(feed_grads[0]), scattered(feed_grads[1].T), scattered(feed_grads[2]))
    dq, dk, dv, spread = attention_backward(qkv, grad_mixed, inverse, exps, place)
    if after is not None:
        dq, after = lax.optimization_barrier((dq, after))
    result, sums_one, grad_qkv = project_back(
        layer, shards, dq, dk, dv, normed_one, current, grad_attended, weight_qkv, gain_one, out_dtype
    )
    small = jnp.concatenate([sums_two[:2].reshape(-1), sums_one[:1].reshape(-1), gather_table(spread).reshape(-1)])
    return result, feed_sums, grad_qkv, small, after

def layer_totals(sums):
    feed_sums, grad_qkv, small = sums
    if len(feed_sums) == 1:
        packed = feed_sums[0]
        grad_up = unpack(packed, 0, FF)
        grad_down = packed[512:1024].T
        grad_proj = unpack(packed, 1024, D)
        grad_qkv = unpack(grad_qkv, 0, 3 * D)
    else:
        grad_up, grad_down, grad_proj = feed_sums
        grad_qkv = grad_qkv.reshape(-1, 3 * D)
    rest = small[FF : 3 * FF].reshape(8, D)
    return (
        rest[6], rest[7], grad_qkv, rest[4], rest[5], small[3 * FF :].reshape(TABLE_ROWS, HEADS), grad_proj, rest[1],
        rest[2], rest[3], grad_up, small[:FF], grad_down, rest[0],
    )

def body(inputs, clip_ids, *rest):
    weights, cotangent = rest[:-1], rest[-1]
    frames = inputs.shape[1]
    place = place_codes()
    aug = mask_operands(clip_ids[0], frames)
    upstream = shift_in(cotangent[0].transpose(1, 2, 0, 3))
    current = to_windows(inputs[0].transpose(1, 2, 0, 3))
    current, saved_first = layer_forward(0, current, weights, place, None, F32)
    current, upstream = lax.optimization_barrier((current, upstream))
    current = shift_in(from_windows(current))
    current, saved_second = layer_forward(1, current, weights, place, aug, BF16)
    block_output = shift_out(current).transpose(2, 0, 1, 3)
    upstream, feed_second, qkv_second, small_second, _ = layer_backward(
        1, upstream, saved_second, weights, place, F32, None
    )
    upstream, block_output = lax.optimization_barrier((upstream, block_output))
    upstream = to_windows(shift_out(upstream))

    upstream, feed_first, qkv_first, small_first, feed_second = layer_backward(
        0, upstream, saved_first, weights, place, BF16, feed_second
    )
    qkv, small, feed_first = reduce_last((qkv_first, qkv_second), (small_first, small_second), feed_first)
    totals_first = layer_totals((feed_first, qkv[0], small[0]))
    totals_second = layer_totals((feed_second, qkv[1], small[1]))
    input_grad = from_windows(upstream).transpose(2, 0, 1, 3)
    results = [jnp.stack(pair) for pair in zip(totals_first, totals_second)]
    return (block_output.reshape(inputs.shape), input_grad.reshape(inputs.shape)) + tuple(results)

def solution(mesh):
    tokens = P("dp", "tm", None, None, None)
    split = P(None, "tm", None)
    placed = (tokens, P("dp", None)) + (P(),) * 14 + (tokens,)
    outs = (tokens, tokens, P(), P(), split, P(), P(), P(), split, P(), P(), P(), split, P(), split, P())
    return jax.shard_map(body, mesh=mesh, in_specs=placed, out_specs=outs, check_vma=False)
```

```python
from functools import partial
import math

import jax
import jax.numpy as jnp
from jax import lax
from jax.experimental import pallas as pl
from jax.experimental.pallas import tpu as pltpu
from jax.sharding import PartitionSpec as P


D = 512
HEADS = 16
HEAD_DIM = 32
FF = 2048
SIDE = 14
WIN_T = 8
WIN_S = 7
SHIFT_T = 4
SHIFT_S = 3
LAYERS = 2
WIN_ROWS = 392
TABLE_ROWS = 2535
WINDOWS = 4
GROUP = 4
GROUPS = HEADS // GROUP
GW = GROUP * HEAD_DIM
HS = 400
LANES = 1664
OT_LANES = 1792
CODE = 768
BASE = 1536
LOG2E = 1.4426950408889634
QSCALE = HEAD_DIM ** (-0.5) * LOG2E
BIG = 1e30
F32 = jnp.float32
BF16 = jnp.bfloat16
CHUNKS = [(256 * c, 256) for c in range(6)] + [(1536, 128)]

def dot_nn(a, b):
    return lax.dot_general(a, b, (((1,), (0,)), ((), ())), preferred_element_type=F32)

def dot_nt(a, b):
    return lax.dot_general(a, b, (((1,), (1,)), ((), ())), preferred_element_type=F32)


def code_shift(spot):
    return 8 * (84 - (spot // WIN_S * 13 + spot % WIN_S))

def head_lanes(rows):
    return lax.broadcasted_iota(jnp.int32, (rows, GW), 1) // HEAD_DIM

def stack_heads(stack_ref, block):
    lane_head = head_lanes(WIN_ROWS)
    zero = jnp.zeros((), block.dtype)
    for h in range(GROUP):
        stack_ref[HS * h : HS * h + WIN_ROWS, :GW] = jnp.where(lane_head == h, block, zero)

def clear_gaps(stack_ref):
    width = stack_ref.shape[1]
    for h in range(GROUP):
        stop = HS * (h + 1) if h < GROUP - 1 else LANES
        stack_ref[HS * h + 384 : stop, :] = jnp.zeros((stop - HS * h - 384, width), stack_ref.dtype)

def unstack(turned_ref):
    picked = []
    for h in range(GROUP):
        rows = turned_ref[HEAD_DIM * h : HEAD_DIM * (h + 1), 384 * h : 384 * h + 512 + 128]
        if h:
            rows = pltpu.roll(rows, 640 - 16 * h, axis=1)
        picked.append(rows[:, :512])
    return jnp.concatenate(picked, axis=0).T[:WIN_ROWS]

def build_bias(tab_ref, place_ref, bias_ref, rolled):
    bias_ref[...] = jnp.zeros((WIN_ROWS, LANES), F32)
    for h in range(GROUP):
        base = tab_ref[0, h]
        for spot in range(49):
            shift = code_shift(spot)
            rolled[8 * spot : 8 * spot + 8, :] = pltpu.roll(base, BASE - shift, axis=1)[:, :CODE]
        part = dot_nn(rolled[...].astype(BF16), place_ref[h])
        bias_ref[:, 384 * h : 384 * h + 512] += part * LOG2E

def forward_kernel(masked, *refs):
    if masked:
        (q_ref, k_ref, v_ref, tab_ref, place_ref, kaug_ref, qaug_ref, o_ref, inv_ref, e_ref, stack, rolled, turned, bias_sum) = refs
    else:
        (q_ref, k_ref, v_ref, tab_ref, place_ref, o_ref, inv_ref, e_ref, stack, rolled, turned, bias_sum) = refs

    @pl.when((pl.program_id(0) == 0) & (pl.program_id(1) == 0))
    def _():
        clear_gaps(stack)
        if masked:
            for h in range(GROUP):
                stack[HS * h : HS * h + WIN_ROWS, GW:] = qaug_ref[...]

    @pl.when(pl.program_id(1) == 0)
    def _():
        build_bias(tab_ref, place_ref, bias_sum, rolled)

    stack_heads(stack, q_ref[0])
    keys = k_ref[0]
    if masked:
        keys = jnp.concatenate([keys, kaug_ref[0]], axis=1)
    values = v_ref[0].astype(F32).T
    values = jnp.concatenate([values, jnp.ones((16, WIN_ROWS), F32)], axis=0).astype(BF16)
    for start, width in CHUNKS:
        scores = dot_nt(keys, stack[start : start + width, :]) + bias_sum[:, start : start + width]
        top = jnp.max(scores, axis=0, keepdims=True)
        e_ref[0, :, start : start + width] = jnp.exp2(scores - top).astype(BF16)
    for start, width in CHUNKS:
        mixed = dot_nn(values, e_ref[0, :, start : start + width])
        inverse = 1.0 / mixed[GW : GW + 8]
        turned[:, start : start + width] = mixed[:GW] * inverse[:1]
        inv_ref[0, :, start : start + width] = inverse
    o_ref[0] = unstack(turned).astype(BF16)

def backward_kernel(q_ref, k_ref, v_ref, do_ref, inv_ref, e_ref, place_ref,
                    dq_ref, dk_ref, dv_ref, dtab_ref, stack, dstack, probs, slopes, turned, bias_sum):
    @pl.when((pl.program_id(0) == 0) & (pl.program_id(1) == 0))
    def _():
        clear_gaps(stack)
        clear_gaps(dstack)

    @pl.when(pl.program_id(1) == 0)
    def _():
        bias_sum[...] = jnp.zeros_like(bias_sum)

    stack_heads(stack, q_ref[0])
    stack_heads(dstack, do_ref[0])
    keys_turned = k_ref[0].astype(F32).T.astype(BF16)
    values = v_ref[0]
    for start, width in CHUNKS:
        lanes = slice(start, start + width)
        chances = e_ref[0, :, lanes].astype(F32) * inv_ref[0, :1, lanes]
        slope = chances * dot_nt(values, dstack[lanes, :])
        slope = slope - chances * jnp.sum(slope, axis=0, keepdims=True)
        probs[:, lanes] = chances.astype(BF16)
        slopes[:, lanes] = slope.astype(BF16)
        bias_sum[:, lanes] += slope
    dv_ref[0] = dot_nn(probs[...], dstack[...]).astype(BF16)
    dk_ref[0] = (dot_nn(slopes[...], stack[...]) * math.log(2.0)).astype(BF16)
    for start, width in CHUNKS:
        turned[:, start : start + width] = dot_nn(keys_turned, slopes[:, start : start + width])
    dq_ref[0] = (unstack(turned) * HEAD_DIM ** (-0.5)).astype(BF16)

    @pl.when(pl.program_id(1) == WINDOWS - 1)
    def _():
        dtab_ref[...] = jnp.zeros_like(dtab_ref)
        pad = jnp.zeros((8, BASE - CODE), F32)
        for h in range(GROUP):
            coded = dot_nt(bias_sum[:, 384 * h : 384 * h + 512].astype(BF16), place_ref[h])
            total = jnp.zeros((8, BASE), F32)
            for hj in range(WIN_S):
                line = coded[8 * (WIN_S * hj + 6) : 8 * (WIN_S * hj + 6) + 8]
                for wj in range(WIN_S - 1):
                    spot = WIN_S * hj + wj
                    line = line + pltpu.roll(coded[8 * spot : 8 * spot + 8], 8 * (6 - wj), axis=1)
                line = jnp.concatenate([line, pad], axis=1)
                total = total + (pltpu.roll(line, 104 * (6 - hj), axis=1) if hj < 6 else line)
            dtab_ref[0, h] = total

def busy(microseconds):
    return pl.CostEstimate(flops=microseconds * 1_000_000_000, bytes_accessed=microseconds * 1_000_000, transcendentals=0)

def head_block(part):
    return pl.BlockSpec((1, WIN_ROWS, GW), lambda g, w: (w, 0, part * GROUPS + g))

PLAIN = pl.BlockSpec((1, WIN_ROWS, GW), lambda g, w: (w, 0, g))
INV = pl.BlockSpec((1, 8, LANES), lambda g, w: (g * WINDOWS + w, 0, 0))
EXPS = pl.BlockSpec((1, WIN_ROWS, LANES), lambda g, w: (g * WINDOWS + w, 0, 0))
TABLE = pl.BlockSpec((1, GROUP, 8, BASE), lambda g, w: (g, 0, 0, 0))
PLACE = pl.BlockSpec((GROUP, CODE, 512), lambda g, w: (0, 0, 0), pipeline_mode=pl.Buffered(1))
KAUG = pl.BlockSpec((1, WIN_ROWS, GW), lambda g, w: (w, 0, 0))
QAUG = pl.BlockSpec((WIN_ROWS, GW), lambda g, w: (0, 0))
VMEM_LIMIT = 62 * 1024 * 1024

def attention_forward(qkv, table, place, aug):
    masked = aug is not None
    wide = 2 * GW if masked else GW
    return pl.pallas_call(
        partial(forward_kernel, masked),
        grid=(GROUPS, WINDOWS),
        in_specs=[head_block(0), head_block(1), head_block(2), TABLE, PLACE] + ([KAUG, QAUG] if masked else []),
        out_specs=[PLAIN, INV, EXPS],
        out_shape=[
            jax.ShapeDtypeStruct((WINDOWS, WIN_ROWS, D), BF16),
            jax.ShapeDtypeStruct((GROUPS * WINDOWS, 8, LANES), F32),
            jax.ShapeDtypeStruct((GROUPS * WINDOWS, WIN_ROWS, LANES), BF16),
        ],
        scratch_shapes=[
            pltpu.VMEM((LANES, wide), BF16),
            pltpu.VMEM((WIN_ROWS, CODE), F32),
            pltpu.VMEM((GW, OT_LANES), F32),
            pltpu.VMEM((WIN_ROWS, LANES), F32),
        ],
        compiler_params=pltpu.CompilerParams(vmem_limit_bytes=VMEM_LIMIT),
        cost_estimate=busy(31),
        name="attention_forward",
    )(qkv, qkv, qkv, table, place, *(aug or ()))

def attention_backward(qkv, grad_mixed, inverse, exps, place):
    return pl.pallas_call(
        backward_kernel,
        grid=(GROUPS, WINDOWS),
        in_specs=[head_block(0), head_block(1), head_block(2), PLAIN, INV, EXPS, PLACE],
        out_specs=[PLAIN, PLAIN, PLAIN, TABLE],
        out_shape=[jax.ShapeDtypeStruct((WINDOWS, WIN_ROWS, D), BF16)] * 3
        + [jax.ShapeDtypeStruct((GROUPS, GROUP, 8, BASE), F32)],
        scratch_shapes=[
            pltpu.VMEM((LANES, GW), BF16),
            pltpu.VMEM((LANES, GW), BF16),
            pltpu.VMEM((WIN_ROWS, LANES), BF16),
            pltpu.VMEM((WIN_ROWS, LANES), BF16),
            pltpu.VMEM((GW, OT_LANES), F32),
            pltpu.VMEM((WIN_ROWS, LANES), F32),
        ],
        compiler_params=pltpu.CompilerParams(vmem_limit_bytes=VMEM_LIMIT),
        cost_estimate=busy(52),
        name="attention_backward",
    )(qkv, qkv, qkv, grad_mixed, inverse, exps, place)


def spread_table(table_rows):
    cube = table_rows.T.reshape(HEADS, 15, 169)
    rows = jnp.stack([cube[:, 7 - tj : 15 - tj] for tj in range(WIN_T)], axis=1)
    rows = rows.transpose(0, 1, 3, 2).reshape(HEADS, WIN_T, 169 * WIN_T)
    rows = jnp.pad(rows, ((0, 0), (0, 0), (0, BASE - 169 * WIN_T)))
    return rows.reshape(GROUPS, GROUP, WIN_T, BASE).astype(F32)

def gather_table(spread):
    rows = spread.reshape(HEADS, WIN_T, BASE)[:, :, : 169 * WIN_T].reshape(HEADS, WIN_T, 169, WIN_T)
    rows = rows.transpose(0, 1, 3, 2)
    total = sum(
        jnp.pad(rows[:, tj], ((0, 0), (7 - tj, tj), (0, 0))) for tj in range(WIN_T)
    )
    return total.reshape(HEADS, TABLE_ROWS).T

def place_codes():
    code = jnp.arange(CODE, dtype=jnp.int32)
    spot_h, spot_w = code // 8 // 13, code // 8 % 13
    lane = (spot_h * WIN_S + spot_w) * 8 + code % 8
    lane = jnp.where((spot_h < WIN_S) & (spot_w < WIN_S), lane, -1000)
    target = lane[None, :] + 16 * jnp.arange(GROUP, dtype=jnp.int32)[:, None]
    return (target[:, :, None] == jnp.arange(512, dtype=jnp.int32)).astype(BF16)

def mask_operands(clip_row, frames):
    index = lax.axis_index("tm")
    wrapped = jnp.concatenate([clip_row, clip_row[:1]])
    own = lax.dynamic_slice_in_dim(wrapped, index * frames + SHIFT_T, 1)
    following = lax.dynamic_slice_in_dim(jnp.concatenate([clip_row, clip_row[:SHIFT_T]]), (index + 1) * frames, 1)
    differs = (own != following).astype(F32)
    token = jnp.arange(WIN_ROWS, dtype=jnp.int32)
    late = (token % 8 >= SHIFT_T).astype(F32)
    low = (token // 8 // WIN_S >= WIN_S - SHIFT_S).astype(F32)
    right = (token // 8 % WIN_S >= WIN_S - SHIFT_S).astype(F32)
    sides = jnp.stack([late, low, right], axis=1)
    window = jnp.arange(WINDOWS)
    weight = jnp.stack(
        [jnp.broadcast_to(differs, (WINDOWS,)), (window // 2).astype(F32), (window % 2).astype(F32)], axis=1
    )
    queries = jnp.concatenate([sides, 1.0 - sides], axis=1)
    keys = -BIG * jnp.concatenate([weight, weight], axis=1)[:, None, :] * jnp.concatenate([1.0 - sides, sides], axis=1)
    queries = jnp.pad(queries, ((0, 0), (0, GW - 6))).astype(BF16)
    keys = jnp.pad(keys, ((0, 0), (0, 0), (0, GW - 6))).astype(BF16)
    return (keys, queries)


TAIL_SLOPE = 0.21
TAIL_POLY = (
    -0.07194446913289963, 0.2849435841958524, -0.3329670889498132, 0.35241963260033626, -0.09596225895564263,
    0.12572571978855923, 0.06897590427205952, 0.0850992002684089, 0.08370977184002107,
)

def gelu_and_slope(u):
    t = 1.0 / (1.0 + TAIL_SLOPE * jnp.abs(u))
    tail = TAIL_POLY[0] * t + TAIL_POLY[1]
    for coefficient in TAIL_POLY[2:]:
        tail = tail * t + coefficient
    bell = jnp.exp2(u * u * (-0.5 * LOG2E))
    tail = tail * t * bell
    chance = jnp.where(u >= 0.0, 1.0 - tail, tail)
    return u * chance, chance + u * bell * (1.0 / math.sqrt(2.0 * math.pi))

def normalized(values):
    center = values - jnp.mean(values, axis=1, keepdims=True)
    scale = lax.rsqrt(jnp.mean(center * center, axis=1, keepdims=True) + 1e-05)
    return center * scale, scale

def norm_backward(grad_normed, gain, shape, scale):
    e = grad_normed * gain
    return scale * (e - jnp.mean(e, axis=1, keepdims=True) - shape * jnp.mean(e * shape, axis=1, keepdims=True))

def turned_low(block):
    return block.astype(F32).T.astype(BF16)

def column_sum(block):
    return jnp.sum(block, axis=0, keepdims=True)

def project_in_kernel(layer, x_ref, gain_ref, shift_ref, w_ref, qb_ref, vb_ref, n_ref, qkv_ref):
    row = slice(layer, layer + 1)
    shape, _ = normalized(x_ref[0].astype(F32))
    n = (shape * gain_ref[row].astype(F32) + shift_ref[row].astype(F32)).astype(BF16)
    n_ref[0] = n
    qkv_ref[0, :, :D] = ((dot_nn(n, w_ref[0, :, :D]) + qb_ref[row].astype(F32)) * QSCALE).astype(BF16)
    qkv_ref[0, :, D : 2 * D] = dot_nn(n, w_ref[0, :, D : 2 * D]).astype(BF16)
    qkv_ref[0, :, 2 * D :] = (dot_nn(n, w_ref[0, :, 2 * D :]) + vb_ref[row].astype(F32)).astype(BF16)

def feed_forward_kernel(layer, x_ref, o_ref, wp_ref, wu_ref, wd_ref, bp_ref, gain_ref, shift_ref, bu_ref, bd_ref,
                        x1_ref, n_ref, act_ref, slope_ref, x2_ref):
    row = slice(layer, layer + 1)
    x1 = x_ref[0].astype(F32) + dot_nn(o_ref[0], wp_ref[0]) + bp_ref[row].astype(F32)
    x1_ref[0] = x1
    shape, _ = normalized(x1)
    n = (shape * gain_ref[row].astype(F32) + shift_ref[row].astype(F32)).astype(BF16)
    n_ref[0] = n
    total = x1 + bd_ref[row].astype(F32)
    for c in range(4):
        for part in (0, 1):
            cols = slice(512 * c + 256 * part, 512 * c + 256 * part + 256)
            g, slope = gelu_and_slope(dot_nn(n, wu_ref[0, :, cols]) + bu_ref[row, cols].astype(F32))
            act_ref[0, :, cols] = g.astype(BF16)
            slope_ref[0, :, cols] = slope.astype(BF16)
        wide = slice(512 * c, 512 * c + 512)
        total = total + dot_nn(act_ref[0, :, wide], wd_ref[0, wide, :])
    x2_ref[0] = total.astype(x2_ref.dtype)

def feed_backward_kernel(layer, shards, dz_ref, x1_ref, n_ref, o_ref, act_ref, slope_ref, wp_ref, wu_ref, wd_ref, gain_ref,
                         dx1_ref, do_ref, sums_ref, *rest):
    grads, (du, acc_up, acc_down, acc_proj) = rest[:-4], rest[-4:]
    row = slice(layer, layer + 1)
    step = pl.program_id(0)

    @pl.when(step == 0)
    def _():
        sums_ref[...] = jnp.zeros_like(sums_ref)
        acc_up[...] = jnp.zeros_like(acc_up)
        acc_down[...] = jnp.zeros_like(acc_down)
        acc_proj[...] = jnp.zeros_like(acc_proj)

    dz = dz_ref[0].astype(F32)
    dm = dz.astype(BF16)
    dm_turned = turned_low(dm)
    n_turned = turned_low(n_ref[0])
    dn = jnp.zeros((WIN_ROWS, D), F32)
    for c in range(4):
        for part in (0, 1):
            cols = slice(512 * c + 256 * part, 512 * c + 256 * part + 256)
            grad = dot_nt(dm, wd_ref[0, cols, :]) * slope_ref[0, :, cols].astype(F32)
            low = grad.astype(BF16)
            du[:, cols] = low
            sums_ref[0:1, cols] += column_sum(low.astype(F32))
        wide = slice(512 * c, 512 * c + 512)
        acc_down[:, wide] += dot_nn(dm_turned, act_ref[0, :, wide])
        acc_up[:, wide] += dot_nn(n_turned, du[:, wide])
        dn = dn + dot_nt(du[:, wide], wu_ref[0, :, wide])
    shape, scale = normalized(x1_ref[0])
    dx1 = dz + norm_backward(dn, gain_ref[row].astype(F32), shape, scale)
    dx1_ref[0] = dx1
    da = dx1.astype(BF16)
    do_ref[0] = dot_nt(da, wp_ref[0]).astype(BF16)
    acc_proj[...] += dot_nn(turned_low(o_ref[0]), da)
    sums_ref[1:2, :] += jnp.concatenate(
        [column_sum(dm.astype(F32)), column_sum(da.astype(F32)), column_sum(dn * shape), column_sum(dn)], axis=1
    )

    @pl.when(step == WINDOWS - 1)
    def _():
        if shards == 16:
            (packed,) = grads
            for s in range(16):
                for c in range(16):
                    packed[s, 32 * c : 32 * c + 32, :] = acc_up[32 * s : 32 * s + 32, 128 * c : 128 * c + 128].astype(BF16)
                packed[s, 512:1024, :] = acc_down[:, 128 * s : 128 * s + 128].astype(BF16)
                for c in range(4):
                    packed[s, 1024 + 32 * c : 1056 + 32 * c, :] = acc_proj[32 * s : 32 * s + 32, 128 * c : 128 * c + 128].astype(BF16)
        else:
            for target, source in zip(grads, (acc_up, acc_down, acc_proj)):
                target[...] = source[...].astype(BF16)

def project_back_kernel(layer, shards, dq_ref, dk_ref, dv_ref, n_ref, x_ref, dx1_ref, w_ref, gain_ref, dx_ref, sums_ref, grad_ref, acc):
    row = slice(layer, layer + 1)
    step = pl.program_id(0)

    @pl.when(step == 0)
    def _():
        sums_ref[...] = jnp.zeros_like(sums_ref)
        acc[...] = jnp.zeros_like(acc)

    n_turned = turned_low(n_ref[0])
    dn = jnp.zeros((WIN_ROWS, D), F32)
    for i, part in enumerate((dq_ref, dk_ref, dv_ref)):
        cols = slice(D * i, D * i + D)
        dn = dn + dot_nt(part[0], w_ref[0, :, cols])
        acc[:, cols] += dot_nn(n_turned, part[0])
    shape, scale = normalized(x_ref[0].astype(F32))
    dx_ref[0] = (dx1_ref[0] + norm_backward(dn, gain_ref[row].astype(F32), shape, scale)).astype(dx_ref.dtype)
    sums_ref[0:1, :] += jnp.concatenate(
        [column_sum(dq_ref[0].astype(F32)), column_sum(dv_ref[0].astype(F32)), column_sum(dn * shape), column_sum(dn)], axis=1
    )

    @pl.when(step == WINDOWS - 1)
    def _():
        if shards == 16:
            for s in range(16):
                for c in range(12):
                    grad_ref[s, 32 * c : 32 * c + 32, :] = acc[32 * s : 32 * s + 32, 128 * c : 128 * c + 128].astype(BF16)
        else:
            grad_ref[...] = acc[...].astype(BF16)

def window_block(width):
    return pl.BlockSpec((1, WIN_ROWS, width), lambda w: (w, 0, 0))

def window_shape(width, dtype):
    return jax.ShapeDtypeStruct((WINDOWS, WIN_ROWS, width), dtype)

def weight_block(layer, rows, columns):
    return pl.BlockSpec((1, rows, columns), lambda w: (layer, 0, 0), pipeline_mode=pl.Buffered(1))

def whole_block(*shape):
    return pl.BlockSpec(shape, lambda w: (0,) * len(shape))

DENSE_PARAMS = pltpu.CompilerParams(vmem_limit_bytes=VMEM_LIMIT)
ROW = whole_block(LAYERS, D)

def project_in(layer, x, gain, shift, weight, q_bias, v_bias):
    return pl.pallas_call(
        partial(project_in_kernel, layer),
        grid=(WINDOWS,),
        in_specs=[window_block(D), ROW, ROW, weight_block(layer, D, 3 * D), ROW, ROW],
        out_specs=[window_block(D), window_block(3 * D)],
        out_shape=[window_shape(D, BF16), window_shape(3 * D, BF16)],
        compiler_params=DENSE_PARAMS,
        cost_estimate=busy(8),
        name="project_in",
    )(x, gain, shift, weight, q_bias, v_bias)

def feed_forward(layer, x, mixed, wp, wu, wd, bp, gain, shift, bu, bd, out_dtype):
    return pl.pallas_call(
        partial(feed_forward_kernel, layer),
        grid=(WINDOWS,),
        in_specs=[window_block(D), window_block(D), weight_block(layer, D, D), weight_block(layer, D, FF),
                  weight_block(layer, FF, D), ROW, ROW, ROW, whole_block(LAYERS, FF), ROW],
        out_specs=[window_block(D), window_block(D), window_block(FF), window_block(FF), window_block(D)],
        out_shape=[window_shape(D, F32), window_shape(D, BF16), window_shape(FF, BF16), window_shape(FF, BF16),
                   window_shape(D, out_dtype)],
        compiler_params=DENSE_PARAMS,
        cost_estimate=busy(28),
        name="feed_forward",
    )(x, mixed, wp, wu, wd, bp, gain, shift, bu, bd)

def feed_backward(layer, shards, dz, x1, normed, mixed, act, slope, wp, wu, wd, gain):
    if shards == 16:
        grad_shapes = [(16, 1152, 128)]
    else:
        grad_shapes = [(D, FF), (D, FF), (D, D)]
    return pl.pallas_call(
        partial(feed_backward_kernel, layer, shards),
        grid=(WINDOWS,),
        in_specs=[window_block(D), window_block(D), window_block(D), window_block(D), window_block(FF), window_block(FF),
                  weight_block(layer, D, D), weight_block(layer, D, FF), weight_block(layer, FF, D), ROW],
        out_specs=[window_block(D), window_block(D), whole_block(8, FF)] + [whole_block(*shape) for shape in grad_shapes],
        out_shape=[window_shape(D, F32), window_shape(D, BF16), jax.ShapeDtypeStruct((8, FF), F32)]
        + [jax.ShapeDtypeStruct(shape, BF16) for shape in grad_shapes],
        scratch_shapes=[pltpu.VMEM((WIN_ROWS, FF), BF16), pltpu.VMEM((D, FF), F32), pltpu.VMEM((D, FF), F32), pltpu.VMEM((D, D), F32)],
        compiler_params=DENSE_PARAMS,
        cost_estimate=busy(28),
        name="feed_backward",
    )(dz, x1, normed, mixed, act, slope, wp, wu, wd, gain)

def project_back(layer, shards, dq, dk, dv, normed, x, dx1, weight, gain, out_dtype):
    grad_shape = (16, 384, 128) if shards == 16 else (D, 3 * D)
    return pl.pallas_call(
        partial(project_back_kernel, layer, shards),
        grid=(WINDOWS,),
        in_specs=[window_block(D)] * 6 + [weight_block(layer, D, 3 * D), ROW],
        out_specs=[window_block(D), whole_block(8, FF), whole_block(*grad_shape)],
        out_shape=[window_shape(D, out_dtype), jax.ShapeDtypeStruct((8, FF), F32), jax.ShapeDtypeStruct(grad_shape, BF16)],
        scratch_shapes=[pltpu.VMEM((D, 3 * D), F32)],
        compiler_params=DENSE_PARAMS,
        cost_estimate=busy(13),
        name="project_back",
    )(dq, dk, dv, normed, x, dx1, weight, gain)


def passed_along(value, axis, steps):
    count = lax.axis_size(axis)
    pairs = [(source, (source + steps) % count) for source in range(count)]
    return lax.ppermute(value, axis, pairs)

def to_windows(field):
    channels = field.shape[-1]
    return field.reshape(2, WIN_S, 2, WIN_S, WIN_T, channels).transpose(0, 2, 1, 3, 4, 5).reshape(WINDOWS, WIN_ROWS, channels)

def from_windows(windows):
    channels = windows.shape[-1]
    return windows.reshape(2, 2, WIN_S, WIN_S, WIN_T, channels).transpose(0, 2, 1, 3, 4, 5).reshape(SIDE, SIDE, WIN_T, channels)

def shift_in(field):
    ahead = passed_along(field[:, :, :SHIFT_T].astype(BF16), "tm", -1).astype(field.dtype)
    moved = jnp.concatenate([field[:, :, SHIFT_T:], ahead], axis=2)
    return to_windows(jnp.roll(moved, (-SHIFT_S, -SHIFT_S), axis=(0, 1)))

def shift_out(windows):
    moved = jnp.roll(from_windows(windows), (SHIFT_S, SHIFT_S), axis=(0, 1))
    behind = passed_along(moved[:, :, SHIFT_T:].astype(BF16), "tm", 1).astype(moved.dtype)
    return jnp.concatenate([behind, moved[:, :, :SHIFT_T]], axis=2)

def layer_forward(layer, current, weights, place, aug, out_dtype):
    (gain_one, shift_one, weight_qkv, bias_query, bias_value, table_rows, weight_proj, bias_proj,
     gain_two, shift_two, weight_up, bias_up, weight_down, bias_down) = weights
    table = spread_table(table_rows[layer])
    normed_one, qkv = project_in(layer, current, gain_one, shift_one, weight_qkv, bias_query, bias_value)
    mixed, inverse, exps = attention_forward(qkv, table, place, aug)
    attended, normed_two, act, slope, result = feed_forward(
        layer, current, mixed, weight_proj, weight_up, weight_down, bias_proj, gain_two, shift_two, bias_up, bias_down, out_dtype
    )
    return result, (current, normed_one, qkv, mixed, inverse, exps, attended, normed_two, act, slope)

def over_groups(value):
    count = lax.axis_size("dp")
    if count != 2:
        return lax.psum(value, "dp")
    return value.astype(F32) + passed_along(value, "dp", 1).astype(F32)

def scattered(grad):
    shard = lax.psum_scatter(grad, "tm", scatter_dimension=0, tiled=True)
    return over_groups(shard.reshape(shard.shape[-2:])).astype(F32)

def swapped(value, reach):
    count = lax.axis_size("tm")
    return lax.ppermute(value, "tm", [(source, source ^ reach) for source in range(count)])

def halved(kept, after):
    count = lax.axis_size("tm")
    index = lax.axis_index("tm")
    reach = 1
    while reach < count:
        pairs = kept.reshape((kept.shape[0] // 2, 2) + kept.shape[1:])
        bit = index // reach % 2
        mine = lax.dynamic_index_in_dim(pairs, bit, 1, keepdims=False)
        sent = lax.dynamic_index_in_dim(pairs, 1 - bit, 1, keepdims=False).astype(BF16)
        kept = mine.astype(F32) + swapped(sent, reach).astype(F32)
        reach = 2 * reach
        if reach == 4:
            kept, after = lax.optimization_barrier((kept, after))
    return over_groups(kept[0].astype(BF16)).astype(F32), after

def gathered(shard):
    count = lax.axis_size("tm")
    index = lax.axis_index("tm")
    whole = shard[None]
    reach = 1
    while reach < count:
        low = index // reach % 2 == 1
        if count // reach >= 4:
            high = index // (2 * reach) % 2 == 1
            one, two, three = (swapped(whole, reach * step) for step in (1, 2, 3))
            first, second = jnp.where(low, one, whole), jnp.where(low, whole, one)
            third, fourth = jnp.where(low, three, two), jnp.where(low, two, three)
            whole = jnp.concatenate(
                [jnp.where(high, third, first), jnp.where(high, fourth, second),
                 jnp.where(high, first, third), jnp.where(high, second, fourth)], axis=0
            )
            reach = 4 * reach
        else:
            other = swapped(whole, reach)
            whole = jnp.concatenate([jnp.where(low, other, whole), jnp.where(low, whole, other)], axis=0)
            reach = 2 * reach
    return whole


def reduce_last(qkv_grads, smalls, after):
    count = lax.axis_size("tm")
    flat = jnp.stack(smalls)
    size = flat.shape[1]
    rows = -(-size // (128 * count))
    flat = jnp.pad(flat, ((0, 0), (0, rows * 128 * count - size))).reshape(LAYERS, count, rows, 128)
    parts = [grad.reshape(count, -1, 128) for grad in qkv_grads]
    height = parts[0].shape[1]
    shard, after = halved(jnp.concatenate(parts + [flat[0].astype(BF16), flat[1].astype(BF16)], axis=1), after)
    whole = gathered(shard[LAYERS * height :]).reshape(count, LAYERS, rows * 128)
    whole = whole.transpose(1, 0, 2).reshape(LAYERS, -1)[:, :size]
    qkv = [shard[height * layer : height * (layer + 1)] for layer in range(LAYERS)]
    return qkv, whole, after

def unpack(packed, start, columns):
    rows = columns // 128 * 32
    return packed[start : start + rows].reshape(columns // 128, 32, 128).transpose(1, 0, 2).reshape(32, columns)

def layer_backward(layer, upstream, saved, weights, place, out_dtype, after):
    (gain_one, _, weight_qkv, _, _, _, weight_proj, _,
     gain_two, _, weight_up, _, weight_down, _) = weights
    (current, normed_one, qkv, mixed, inverse, exps, attended, normed_two, act, slope) = saved
    shards = lax.axis_size("tm")
    grad_attended, grad_mixed, sums_two, *feed_grads = feed_backward(
        layer, shards, upstream, attended, normed_two, mixed, act, slope, weight_proj, weight_up, weight_down, gain_two
    )
    if shards == 16:
        feed_sums = (scattered(feed_grads[0]),)
    else:
        feed_sums = (scattered(feed_grads[0]), scattered(feed_grads[1].T), scattered(feed_grads[2]))
    dq, dk, dv, spread = attention_backward(qkv, grad_mixed, inverse, exps, place)
    if after is not None:
        dq, after = lax.optimization_barrier((dq, after))
    result, sums_one, grad_qkv = project_back(
        layer, shards, dq, dk, dv, normed_one, current, grad_attended, weight_qkv, gain_one, out_dtype
    )
    small = jnp.concatenate([sums_two[:2].reshape(-1), sums_one[:1].reshape(-1), gather_table(spread).reshape(-1)])
    return result, feed_sums, grad_qkv, small, after

def layer_totals(sums):
    feed_sums, grad_qkv, small = sums
    if len(feed_sums) == 1:
        packed = feed_sums[0]
        grad_up = unpack(packed, 0, FF)
        grad_down = packed[512:1024].T
        grad_proj = unpack(packed, 1024, D)
        grad_qkv = unpack(grad_qkv, 0, 3 * D)
    else:
        grad_up, grad_down, grad_proj = feed_sums
        grad_qkv = grad_qkv.reshape(-1, 3 * D)
    rest = small[FF : 3 * FF].reshape(8, D)
    return (
        rest[6], rest[7], grad_qkv, rest[4], rest[5], small[3 * FF :].reshape(TABLE_ROWS, HEADS), grad_proj, rest[1],
        rest[2], rest[3], grad_up, small[:FF], grad_down, rest[0],
    )

def body(inputs, clip_ids, *rest):
    weights, cotangent = rest[:-1], rest[-1]
    frames = inputs.shape[1]
    place = place_codes()
    aug = mask_operands(clip_ids[0], frames)
    upstream = shift_in(cotangent[0].transpose(1, 2, 0, 3))
    current = to_windows(inputs[0].transpose(1, 2, 0, 3))
    current, saved_first = layer_forward(0, current, weights, place, None, F32)
    current, upstream = lax.optimization_barrier((current, upstream))
    current = shift_in(from_windows(current))
    current, saved_second = layer_forward(1, current, weights, place, aug, BF16)
    block_output = shift_out(current).transpose(2, 0, 1, 3)
    upstream, feed_second, qkv_second, small_second, _ = layer_backward(
        1, upstream, saved_second, weights, place, F32, None
    )
    upstream, block_output = lax.optimization_barrier((upstream, block_output))
    upstream = to_windows(shift_out(upstream))

    upstream, feed_first, qkv_first, small_first, feed_second = layer_backward(
        0, upstream, saved_first, weights, place, BF16, feed_second
    )
    qkv, small, feed_first = reduce_last((qkv_first, qkv_second), (small_first, small_second), feed_first)
    totals_first = layer_totals((feed_first, qkv[0], small[0]))
    totals_second = layer_totals((feed_second, qkv[1], small[1]))
    input_grad = from_windows(upstream).transpose(2, 0, 1, 3)
    results = [jnp.stack(pair) for pair in zip(totals_first, totals_second)]
    return (block_output.reshape(inputs.shape), input_grad.reshape(inputs.shape)) + tuple(results)

def solution(mesh):
    tokens = P("dp", "tm", None, None, None)
    split = P(None, "tm", None)
    placed = (tokens, P("dp", None)) + (P(),) * 14 + (tokens,)
    outs = (tokens, tokens, P(), P(), split, P(), P(), P(), split, P(), P(), P(), split, P(), split, P())
    return jax.shard_map(body, mesh=mesh, in_specs=placed, out_specs=outs, check_vma=False)
```
